512 devices in a mesh: rep: 2 (over y), seq: 128 (over x, z), head: 2 (over core).
Axes of the slice: x: 8, y: 2, z: 16, core: 2. Of those that a mesh axis runs over, the one named last changes fastest.
The devices are a block of a 8x8x16 slice.
Arguments:
- prompt_query: bfloat16 [32768, 1792], P(('rep', 'seq', 'head')), parts along dimension 0, may hold values from -12 to 12
- prompt_key: bfloat16 [32768, 256], P(('rep', 'seq', 'head')), parts along dimension 0, may hold values from -12 to 12
- prompt_value: bfloat16 [32768, 256], P(('rep', 'seq', 'head')), parts along dimension 0, may hold values from -24 to 24
- prompt_length: int32 [2], P('rep'), parts along dimension 0, may hold values from 8192 to 16384
- span_order: int32 [512], P('rep'), parts along dimension 0, may hold values from 0 to 255, each once
- new_query: bfloat16 [32, 1792], P('rep', 'head'), parts along dimension 0, may hold values from -12 to 12
- new_key: bfloat16 [32, 256], P('rep', 'head'), parts along dimension 0, may hold values from -12 to 12
- new_value: bfloat16 [32, 256], P('rep', 'head'), parts along dimension 0, may hold values from -24 to 24
- cache_key: bfloat16 [32, 2, 32768, 128], P('rep', 'head', 'seq'), parts along dimension 0, may hold values from -12 to 12
- cache_value: bfloat16 [32, 2, 32768, 128], P('rep', 'head', 'seq'), parts along dimension 0, may hold values from -24 to 24
- cache_length: int32 [32], P('rep'), parts along dimension 0, may hold values from 16640 to 32768
Outputs:
- prompt_attended: bfloat16 [32768, 1792], P(('rep', 'seq', 'head')), parts along dimension 0
- decode_attended: bfloat16 [32, 1792], P('rep', 'head'), parts along dimension 0
The draws below stay inside these ranges and needn't reach their ends.
There are 2 independent parts, one for each index of `rep`. The reference program is written for one: setup_inputs(seed, part) draws one part's arguments, and reference() takes and returns one part's arrays. A program takes and returns all parts, laid end to end along the dimension named above; each array names one. Nothing has to cross between parts.
Inputs may be any that keep to these rules, and one draw needn't show every extreme that they name: `span_order`: each of the 256 spans stands once.
All inputs are finite; a program needn't handle non-finite values.
Results may differ from the reference program's by a relative error of at most 0.0045.
Values may be sent and summed in bfloat16 or wider, within the bound.
A program may use at most 128 MiB of HBM per device.

```python
import math
import jax
import jax.numpy as jnp
from jax import lax

HD = 128
QH = 14
KVH = 2
SPAN = 64
SESS = 16
CTX_DEV = 256
NCHUNK = 256
PROMPT = 16384
CTX = 32768


def prompt_fields(key):
    query_key = jax.random.fold_in(key, 31)
    keys_key = jax.random.fold_in(key, 32)
    broad_key = jax.random.fold_in(key, 34)
    row_ids = jnp.arange(PROMPT, dtype=jnp.int32)
    queries = 1.2 * jnp.clip(jax.random.normal(query_key, (PROMPT, QH * HD), jnp.float32), -6.0, 6.0)
    broad = jax.random.uniform(broad_key, (PROMPT, QH * HD), jnp.float32, -6.0, 6.0)
    broad_rows = row_ids % 64 == 5
    queries = jnp.where(broad_rows[:, None], broad, queries)
    keys_drawn = 1.2 * jnp.clip(jax.random.normal(keys_key, (PROMPT, KVH * HD), jnp.float32), -6.0, 6.0)
    return (queries, keys_drawn)


def decode_fields(key):
    query_key = jax.random.fold_in(key, 41)
    keys_key = jax.random.fold_in(key, 42)
    broad_key = jax.random.fold_in(key, 44)
    session_ids = jnp.arange(SESS, dtype=jnp.int32)
    queries = 1.2 * jnp.clip(jax.random.normal(query_key, (SESS, QH * HD), jnp.float32), -6.0, 6.0)
    broad = jax.random.uniform(broad_key, (SESS, QH * HD), jnp.float32, -6.0, 6.0)
    broad_rows = session_ids % 4 == 1
    queries = jnp.where(broad_rows[:, None], broad, queries)
    keys_drawn = 1.2 * jnp.clip(jax.random.normal(keys_key, (SESS, KVH, CTX, HD), jnp.float32), -6.0, 6.0)
    far_slot = CTX // 2 + CTX_DEV // 2
    planted_scale = 5.0 / (1.44 * math.sqrt(HD))
    leading = queries.reshape(SESS, KVH, QH // KVH, HD)[:, :, 0, :]
    keys_drawn = keys_drawn.at[:, :, far_slot, :].set(planted_scale * leading)
    return (queries, keys_drawn)


def draw_prompt_query(key, part):
    return prompt_fields(key)[0].astype(jnp.bfloat16)


def draw_prompt_key(key, part):
    return prompt_fields(key)[1].astype(jnp.bfloat16)


def draw_new_query(key, part):
    return decode_fields(key)[0].astype(jnp.bfloat16)


def draw_cache_key(key, part):
    return decode_fields(key)[1].astype(jnp.bfloat16)


def plant(values, key, low, top_value):
    longest = values.shape.index(max(values.shape))
    spots = []
    for shift in (0, 1):
        where = [jax.random.randint(jax.random.fold_in(key, axis), (), 0, length) for axis, length in enumerate(values.shape)]
        where[longest] = (where[longest] + shift) % values.shape[longest]
        spots.append(tuple(where))
    return values.at[spots[0]].set(low).at[spots[1]].set(top_value)


def level_of(key, shape, split, least, high):
    factor_of = 1.0
    for position, shards_of in split:
        draws = jax.random.uniform(jax.random.fold_in(jax.random.fold_in(key, 6), position), (shards_of,), jnp.float32, least / len(split), high / len(split))
        factor_of = factor_of * jnp.repeat(jnp.exp(draws), shape[position] // shards_of).reshape((-1,) + (1,) * (len(shape) - 1 - position))
    return factor_of


def scatter_about(key, shape, width, most, shards=(), kind=jnp.bfloat16):
    values = jax.random.normal(key, shape, jnp.float32) * width
    if len(shards) > 0:
        values = level_of(key, shape, shards, -0.22, 0.18) * values
    return jnp.clip(values, min=-most, max=most).astype(kind)


def setup_inputs(seed: int = 0, part: int = 0) -> dict:
    keys = jax.random.split(jax.random.key(seed), 12)
    part_splits = jax.random.split(jax.random.fold_in(keys[11], part), 12)
    return {
        "prompt_query": draw_prompt_query(jax.random.fold_in(jax.random.fold_in(keys[11], part), 71), part),
        "prompt_key": draw_prompt_key(jax.random.fold_in(jax.random.fold_in(keys[11], part), 71), part),
        "prompt_value": scatter_about(part_splits[2], (PROMPT, KVH * HD), 4.0, 24.0, ((0, 256),)),
        "prompt_length": jax.random.randint(part_splits[3], (1,), PROMPT // 2, PROMPT + 1).astype(jnp.int32),
        "span_order": jax.random.permutation(part_splits[4], NCHUNK).astype(jnp.int32),
        "new_query": draw_new_query(jax.random.fold_in(jax.random.fold_in(keys[11], part), 71), part),
        "new_key": scatter_about(part_splits[6], (SESS, KVH * HD), 2.0, 12.0, ((1, 2),)),
        "new_value": scatter_about(part_splits[7], (SESS, KVH * HD), 4.0, 24.0, ((1, 2),)),
        "cache_key": draw_cache_key(jax.random.fold_in(jax.random.fold_in(keys[11], part), 71), part),
        "cache_value": scatter_about(part_splits[9], (SESS, KVH, CTX, HD), 4.0, 24.0, ((1, 2), (2, 128))),
        "cache_length": plant(jax.random.randint(part_splits[10], (SESS,), CTX // 2 + CTX_DEV, CTX + 1), jax.random.fold_in(part_splits[10], 1), CTX // 2 + CTX_DEV, CTX).astype(jnp.int32),
    }


def reference(prompt_query, prompt_key, prompt_value, prompt_length, span_order, new_query, new_key, new_value, cache_key, cache_value, cache_length):
    head_group = QH // KVH
    score_scale = 1.0 / math.sqrt(HD)
    row_ids = jnp.arange(PROMPT, dtype=jnp.int32)
    positions = (span_order[row_ids // SPAN] * SPAN + row_ids % SPAN).astype(jnp.int32)
    length_limit = prompt_length[0]
    key_table = prompt_key.astype(jnp.float32).reshape(PROMPT, KVH, HD)
    value_table = prompt_value.astype(jnp.float32).reshape(PROMPT, KVH, HD)
    key_live = positions < length_limit
    block_rows = math.gcd(PROMPT, 256)

    def one_block(block_index):
        start_row = (block_index * block_rows).astype(jnp.int32)
        queries = lax.dynamic_slice_in_dim(prompt_query, start_row, block_rows, 0).astype(jnp.float32)
        queries = queries.reshape(block_rows, KVH, head_group, HD)
        query_pos = lax.dynamic_slice_in_dim(positions, start_row, block_rows, 0)
        scores = jnp.einsum('rkgd,nkd->kgrn', queries, key_table) * score_scale
        allowed = (positions[None, :] <= query_pos[:, None]) & key_live[None, :]
        scores = jnp.where(allowed, scores, -1e+30)
        row_max = lax.optimization_barrier(jnp.max(scores, axis=-1, keepdims=True))
        weights = jnp.where(allowed, jnp.exp(scores - row_max), 0.0)
        row_total = lax.optimization_barrier(jnp.sum(weights, axis=-1))
        rounded = lax.optimization_barrier(weights.astype(jnp.bfloat16)).astype(jnp.float32)
        weighted = jnp.einsum('kgrn,nkd->rkgd', rounded, value_table)
        result = weighted / jnp.transpose(row_total, (2, 0, 1))[..., None]
        result = jnp.where((query_pos < length_limit)[:, None, None, None], result, 0.0)
        return result.reshape(block_rows, QH * HD).astype(jnp.bfloat16)
    prompt_attended = lax.map(one_block, jnp.arange(PROMPT // block_rows, dtype=jnp.int32)).reshape(PROMPT, QH * HD)
    cache_pos = jnp.arange(CTX, dtype=jnp.int32)

    def one_session(session):
        queries = new_query[session].astype(jnp.float32).reshape(KVH, head_group, HD)
        keys_here = cache_key[session].astype(jnp.float32)
        values_here = cache_value[session].astype(jnp.float32)
        fresh_key = new_key[session].astype(jnp.float32).reshape(KVH, HD)
        fresh_value = new_value[session].astype(jnp.float32).reshape(KVH, HD)
        valid = cache_pos < cache_length[session]
        scores = jnp.einsum('kgd,ktd->kgt', queries, keys_here) * score_scale
        scores = jnp.where(valid[None, None, :], scores, -1e+30)
        own_score = jnp.einsum('kgd,kd->kg', queries, fresh_key) * score_scale
        row_max = jnp.maximum(lax.optimization_barrier(jnp.max(scores, axis=-1)), own_score)
        weights = jnp.where(valid[None, None, :], jnp.exp(scores - row_max[..., None]), 0.0)
        own_weight = jnp.exp(own_score - row_max)
        row_total = lax.optimization_barrier(jnp.sum(weights, axis=-1)) + own_weight
        rounded = lax.optimization_barrier(weights.astype(jnp.bfloat16)).astype(jnp.float32)
        own_rounded = lax.optimization_barrier(own_weight.astype(jnp.bfloat16)).astype(jnp.float32)
        weighted = jnp.einsum('kgt,ktd->kgd', rounded, values_here) + own_rounded[..., None] * fresh_value[:, None, :]
        return (weighted / row_total[..., None]).reshape(QH * HD).astype(jnp.bfloat16)
    decode_attended = lax.map(one_session, jnp.arange(SESS, dtype=jnp.int32))
    return (prompt_attended, decode_attended)
```

```python
import heapq
import math

import jax
import jax.numpy as jnp
import numpy as np
from jax import lax
from jax.experimental import pallas as pl
from jax.experimental.pallas import tpu as pltpu
from jax.sharding import Mesh
from jax.sharding import PartitionSpec as P

HD = 128
QH = 14
KVH = 2
GROUP = QH // KVH
SEQ = ("seq_0", "seq_1")
REP_SEQ_HEAD = ("rep", "seq_0", "seq_1", "head")
TILE = 8
NEG = -1e30
MESH = pl.DeviceIdType.MESH


def build_flow(n1, n2):
    half1, half2 = n1 // 2, n2 // 2
    members = {0: [0], half1: [-half1]}
    for k in range(1, half1):
        members[k] = [-k, k]
    heap, free, seq, arrived = [], {}, [0], {}
    order, first, sends = [], [], {}

    def send(now, link, item, into):
        units = len(members[item[2]]) if item[0] == 2 else 1
        begin = max(now, free.get(link, 0.0))
        free[link] = begin + units * (0.75 if link[0] == 2 else 1.4)
        seq[0] += 1
        heapq.heappush(heap, (free[link] + 2.5, seq[0], item))
        into.append(item)

    def phase2(now, k, into):
        for way in (1, -1):
            send(now, (2, way), (2, way, k, -way), into)

    for way in (1, -1):
        send(0.0, (1, way), (1, way, -way, 0), first)
    phase2(0.0, 0, first)
    groups = [(0, 0)]
    while heap:
        now, _, item = heapq.heappop(heap)
        order.append(item)
        into = sends.setdefault(item, [])
        ring, way, which, off2 = item
        if ring == 1:
            dist, k = abs(which), abs(which)
            if dist + 1 <= (half1 if way == 1 else half1 - 1):
                send(now, (1, way), (1, way, which - way, 0), into)
            arrived[k] = arrived.get(k, 0) + 1
            if arrived[k] == len(members[k]):
                groups.append((k, 0))
                phase2(now, k, into)
        else:
            dist = abs(off2)
            groups.append((which, off2))
            last = dist + 1 == half2 and way == (1 if which % 2 == 0 else -1)
            if dist + 1 < half2 or last:
                send(now, (2, way), (2, way, which, off2 - way), into)
    slot, offsets = {}, []
    for k, off2 in groups:
        slot[(k, off2)] = len(offsets)
        offsets.extend((m, off2) for m in members[k])

    def place(item):
        ring, _, which, off2 = item
        if ring == 2:
            return slot[(which, off2)], len(members[which])
        return slot[(abs(which), 0)] + members[abs(which)].index(which), 1

    number = {item: i for i, item in enumerate(order)}

    def resolve(items):
        out = []
        for item in items:
            ring, way, which, off2 = item
            source = (1, way, which + way, 0) if ring == 1 else (2, way, which, off2 + way)
            if ring == 1 and source[2] == 0:
                src = slot[(0, 0)]
            else:
                src = place(source)[0]
            dst, count = place(item)
            out.append((ring, way, src, dst, count, number[item]))
        return out

    steps, total = [], len(offsets) // TILE
    events = [(place(item), resolve(sends[item]), number[item]) for item in order]
    at, filled = 0, {0}
    for tile in range(total):
        need = set(range(tile * TILE, (tile + 1) * TILE))
        mine = []
        while not need <= filled:
            (dst, count), todo, sem = events[at]
            filled.update(range(dst, dst + count))
            mine.append((dst, count, todo, sem))
            at += 1
        steps.append(mine)
    assert at == len(events) and len(offsets) == n1 * n2
    return offsets, resolve(first), steps, len(events)


def prompt_kernel(
    flows,
    sizes,
    span_ref,
    limit_ref,
    q_ref,
    bias_ref,
    k_ref,
    v_ref,
    out_ref,
    buf,
    q_s,
    acc,
    top,
    tot,
    local_sem,
    recv_sem,
    send_sem,
    pair_recv,
    pair_send,
):
    n_x, n_z = sizes
    rows = q_ref.shape[0]
    x, z, core = lax.axis_index("seq_0"), lax.axis_index("seq_1"), lax.axis_index("head")
    steps = len(flows[0][2])
    names = ("seq_0", "seq_1")
    here = (x, z)
    extent = (n_x, n_z)

    def target(dim, way):
        return {names[dim]: lax.rem(here[dim] + way + extent[dim], extent[dim])}

    partner = {"head": 1 - core}
    in_k = pltpu.make_async_copy(k_ref, buf.at[0, 0, :, : KVH * HD], local_sem.at[0])
    in_v = pltpu.make_async_copy(v_ref, buf.at[0, 0, :, KVH * HD :], local_sem.at[1])
    in_k.start()
    in_v.start()
    barrier = pltpu.get_barrier_semaphore()
    for dim in (0, 1):
        for way in (1, -1):
            pl.semaphore_signal(barrier, inc=1, device_id=target(dim, way), device_id_type=MESH)
    pl.semaphore_signal(barrier, inc=1, device_id=partner, device_id_type=MESH)
    in_k.wait()
    in_v.wait()
    pl.semaphore_wait(barrier, 5)

    def ring_copy(flow, send):
        ring, way, src, dst, count, sem = send
        dim = (ring - 1) if flow == 0 else (2 - ring)
        return pltpu.make_async_remote_copy(
            src_ref=buf.at[0, pl.ds(src, count)],
            dst_ref=buf.at[0, pl.ds(dst, count)],
            send_sem=send_sem.at[0],
            recv_sem=recv_sem.at[sem],
            device_id=target(dim, way),
            device_id_type=MESH,
        )

    def pair_copy(tile):
        return pltpu.make_async_remote_copy(
            src_ref=buf.at[0, pl.ds(tile * TILE, TILE)],
            dst_ref=buf.at[1, pl.ds(tile * TILE, TILE)],
            send_sem=pair_send.at[0],
            recv_sem=pair_recv.at[tile],
            device_id=partner,
            device_id_type=MESH,
        )

    for flow in (0, 1):

        @pl.when(core == flow)
        def _():
            for send in flows[flow][1]:
                ring_copy(flow, send).start()

    scale = math.log2(math.e) / math.sqrt(HD)

    row = lax.broadcasted_iota(jnp.int32, (rows, rows), 0)
    col = lax.broadcasted_iota(jnp.int32, (rows, rows), 1)
    tri = jnp.concatenate([jnp.where(col <= row, 0.0, NEG).astype(jnp.float32)] * GROUP, axis=0)
    for g in range(KVH):
        for h in range(GROUP):
            head = g * GROUP + h
            q_s[g, h * rows : (h + 1) * rows, :] = q_ref[:, head * HD : (head + 1) * HD]
        key = buf[0, 0, :, g * HD : (g + 1) * HD]
        value = buf[0, 0, :, (KVH + g) * HD : (KVH + g + 1) * HD]
        s = lax.dot_general(q_s[g], key, (((1,), (1,)), ((), ())), preferred_element_type=jnp.float32)
        s = s + tri
        m = jnp.max(s, axis=1, keepdims=True)
        p = jnp.exp2((s - m) * scale)
        top[g] = jnp.broadcast_to(m, (GROUP * rows, HD))
        total = jnp.sum(p, axis=1, keepdims=True)
        lane = lax.broadcasted_iota(jnp.int32, (GROUP * rows, HD), 1)
        tot[g] = jnp.where(lane == 0, total, 0.0)
        acc[g] = jnp.dot(p.astype(jnp.bfloat16), value, preferred_element_type=jnp.float32)

    keys = TILE * rows

    def attend(side, tile):
        at = pl.ds(tile * TILE, TILE)
        bias = bias_ref[side * steps + tile]
        for g in range(KVH):
            key = buf[side, at, :, g * HD : (g + 1) * HD].reshape(keys, HD)
            value = buf[side, at, :, (KVH + g) * HD : (KVH + g + 1) * HD].reshape(keys, HD)
            s = lax.dot_general(
                q_s[g], key, (((1,), (1,)), ((), ())), preferred_element_type=jnp.float32
            )
            s = s + bias
            m_old = top[g]
            m = jnp.maximum(m_old, jnp.max(s, axis=1, keepdims=True))
            factor = jnp.exp2((m_old - m) * scale)
            m_wide = jnp.concatenate([m] * (keys // HD), axis=1)
            p = jnp.exp2((s - m_wide) * scale)
            part = p[:, :HD]
            for b in range(1, keys // HD):
                part = part + p[:, b * HD : (b + 1) * HD]
            top[g] = m
            tot[g] = tot[g] * factor + part
            acc[g] = acc[g] * factor + jnp.dot(
                p.astype(jnp.bfloat16), value, preferred_element_type=jnp.float32
            )

    def step(j, carry):
        for flow in (0, 1):
            for jj in range(steps):

                @pl.when((core == flow) & (j == jj))
                def _():
                    for dst, count, todo, sem in flows[flow][2][jj]:
                        pltpu.make_async_remote_copy(
                            src_ref=buf.at[0, pl.ds(dst, count)],
                            dst_ref=buf.at[0, pl.ds(dst, count)],
                            send_sem=send_sem.at[0],
                            recv_sem=recv_sem.at[sem],
                            device_id=partner,
                            device_id_type=MESH,
                        ).wait_recv()
                        for send in todo:
                            ring_copy(flow, send).start()

        pair_copy(j).start()
        attend(0, j)

        @pl.when(j > 0)
        def _():
            pair_copy(j - 1).wait_recv()
            attend(1, j - 1)

        return carry

    lax.fori_loop(0, steps, step, 0)
    pair_copy(steps - 1).wait_recv()
    attend(1, steps - 1)

    chips = n_x * n_z
    pltpu.make_async_remote_copy(
        src_ref=buf.at[0, pl.ds(0, chips - 1)],
        dst_ref=buf.at[0, pl.ds(0, chips - 1)],
        send_sem=send_sem.at[0],
        recv_sem=recv_sem.at[0],
        device_id=partner,
        device_id_type=MESH,
    ).wait_send()
    pltpu.make_async_remote_copy(
        src_ref=buf.at[0, pl.ds(0, chips)],
        dst_ref=buf.at[1, pl.ds(0, chips)],
        send_sem=pair_send.at[0],
        recv_sem=recv_sem.at[0],
        device_id=partner,
        device_id_type=MESH,
    ).wait_send()

    me = (x * n_z + z) * 2 + core
    position = span_ref[me] * rows + lax.broadcasted_iota(jnp.int32, (rows, HD), 0)
    live = position < limit_ref[0]
    for g in range(KVH):
        for h in range(GROUP):
            head = g * GROUP + h
            at = slice(h * rows, (h + 1) * rows)
            total = jnp.sum(tot[g, at, :], axis=1, keepdims=True)
            result = jnp.where(live, acc[g, at, :] / total, 0.0)
            out_ref[:, head * HD : (head + 1) * HD] = result.astype(jnp.bfloat16)


def prompt_attention(prompt_query, prompt_key, prompt_value, prompt_length, span_order):
    rows = prompt_query.shape[0]
    n_x, n_z = lax.axis_size("seq_0"), lax.axis_size("seq_1")
    x, z, core = lax.axis_index("seq_0"), lax.axis_index("seq_1"), lax.axis_index("head")
    flow_a = build_flow(n_x, n_z)
    flow_b = build_flow(n_z, n_x)
    flows = (flow_a, flow_b)
    steps = len(flow_a[2])
    off = np.array(
        [[[a, b] for a, b in flow_a[0]], [[b, a] for a, b in flow_b[0]]], np.int32
    )
    order = jnp.where(core == 0, off, off[::-1])
    which = jnp.stack([core, 1 - core]).astype(jnp.int32)
    at_x = (order[..., 0] + x + n_x) % n_x
    at_z = (order[..., 1] + z + n_z) % n_z
    index = ((at_x * n_z + at_z) * 2 + which[:, None]).reshape(-1)
    me = (x * n_z + z) * 2 + core
    numbers = jnp.arange(span_order.shape[0], dtype=jnp.int32)
    picked = jnp.sum(jnp.where(index[:, None] == numbers[None, :], span_order[None, :], 0), axis=1)
    own = jnp.sum(jnp.where(me == numbers, span_order, 0))
    bias = jnp.where(picked < own, 0.0, NEG).astype(jnp.float32)
    bias = jnp.broadcast_to(bias[:, None], (bias.shape[0], rows)).reshape(2 * steps, 1, TILE * rows)
    width = 2 * KVH * HD
    sems = max(flow_a[3], flow_b[3])
    return pl.pallas_call(
        lambda *refs: prompt_kernel(flows, (n_x, n_z), *refs),
        out_shape=jax.ShapeDtypeStruct(prompt_query.shape, jnp.bfloat16),
        in_specs=[
            pl.BlockSpec(memory_space=pltpu.SMEM),
            pl.BlockSpec(memory_space=pltpu.SMEM),
            pl.BlockSpec(memory_space=pltpu.VMEM),
            pl.BlockSpec(memory_space=pltpu.VMEM),
            pl.BlockSpec(memory_space=pl.ANY),
            pl.BlockSpec(memory_space=pl.ANY),
        ],
        out_specs=pl.BlockSpec(memory_space=pltpu.VMEM),
        scratch_shapes=[
            pltpu.VMEM((2, n_x * n_z, rows, width), jnp.bfloat16),
            pltpu.VMEM((KVH, GROUP * rows, HD), jnp.bfloat16),
            pltpu.VMEM((KVH, GROUP * rows, HD), jnp.float32),
            pltpu.VMEM((KVH, GROUP * rows, HD), jnp.float32),
            pltpu.VMEM((KVH, GROUP * rows, HD), jnp.float32),
            pltpu.SemaphoreType.DMA((2,)),
            pltpu.SemaphoreType.DMA((sems,)),
            pltpu.SemaphoreType.DMA((1,)),
            pltpu.SemaphoreType.DMA((steps,)),
            pltpu.SemaphoreType.DMA((1,)),
        ],
        compiler_params=pltpu.CompilerParams(
            collective_id=0, has_side_effects=True, vmem_limit_bytes=48 * 1024 * 1024
        ),
        name="prompt_attention",
    )(span_order, prompt_length, prompt_query, bias, prompt_key, prompt_value)


def gathered_once(array, axis):
    leaves = jax.tree.leaves(array)
    order = sorted(range(len(leaves)), key=lambda k: -leaves[k].size)
    width = (1, *leaves[order[0]].shape)[-1]
    lines = [
        jnp.pad(leaves[k].reshape(-1), (0, -leaves[k].size % width)).reshape(-1, width)
        for k in order
    ]
    both, at, found = (lax.all_gather(jnp.concatenate(lines), axis), 0, {})
    for k, line in zip(order, lines):
        piece = both[:, at : at + len(line)].reshape(len(both), -1)
        found[k] = piece[:, : leaves[k].size].reshape(-1, *leaves[k].shape)
        at += len(line)
    numbers = iter(range(len(leaves)))
    return jax.tree.map(lambda _: found[next(numbers)], array)


def combined_by_axis(array, axes, combine):
    for axis in axes:
        pieces = gathered_once(array, axis)
        array = jax.tree.map(lambda part: part[0], pieces)
        for k in range(1, lax.axis_size(axis)):
            array = combine(array, jax.tree.map(lambda part: part[k], pieces))
    return array


def combine_parts(left, right):
    left_max, left_total, left_weighted = left
    right_max, right_total, right_weighted = right
    joint = jnp.maximum(left_max, right_max)
    left_factor = jnp.exp(left_max - joint)
    right_factor = jnp.exp(right_max - joint)
    return (
        joint,
        left_total * left_factor + right_total * right_factor,
        left_weighted * left_factor[..., None] + right_weighted * right_factor[..., None],
    )


def per_device(
    prompt_query,
    prompt_key,
    prompt_value,
    prompt_length,
    span_order,
    new_query,
    new_key,
    new_value,
    cache_key,
    cache_value,
    cache_length,
):
    head_group = QH // KVH
    score_scale = 1.0 / math.sqrt(HD)
    prompt_attended = prompt_attention(
        prompt_query, prompt_key, prompt_value, prompt_length, span_order
    )
    sessions = new_query.shape[0]
    local_heads = cache_key.shape[1]
    local_ctx = cache_key.shape[2]
    dec_queries = new_query.reshape(sessions, local_heads, head_group, HD)
    cache_pos = lax.axis_index(SEQ) * local_ctx + jnp.arange(local_ctx, dtype=jnp.int32)
    valid = (cache_pos[None, :] < cache_length[:, None])[:, None, None, :]
    scores = (
        jnp.einsum("skgd,sktd->skgt", dec_queries, cache_key, preferred_element_type=jnp.float32)
        * score_scale
    )
    scores = jnp.where(valid, scores, -1e30)
    row_max = jnp.max(scores, axis=-1)
    weights = jnp.where(valid, jnp.exp(scores - row_max[..., None]), 0.0)
    row_total = jnp.sum(weights, axis=-1)
    weighted = jnp.einsum(
        "skgt,sktd->skgd",
        weights.astype(jnp.bfloat16),
        cache_value,
        preferred_element_type=jnp.float32,
    )
    row_max, row_total, weighted = combined_by_axis(
        (row_max, row_total, weighted), SEQ, combine_parts
    )
    own_score = (
        jnp.einsum(
            "skgd,skd->skg",
            dec_queries,
            new_key.reshape(sessions, local_heads, HD),
            preferred_element_type=jnp.float32,
        )
        * score_scale
    )
    final_max = jnp.maximum(row_max, own_score)
    old_factor = jnp.exp(row_max - final_max)
    own_weight = jnp.exp(own_score - final_max)
    row_total = row_total * old_factor + own_weight
    own_rounded = lax.optimization_barrier(own_weight.astype(jnp.bfloat16)).astype(jnp.float32)
    fresh_value = new_value.reshape(sessions, local_heads, 1, HD).astype(jnp.float32)
    weighted = weighted * old_factor[..., None] + own_rounded[..., None] * fresh_value
    decode_attended = (weighted / row_total[..., None]).reshape(sessions, -1).astype(jnp.bfloat16)
    return (prompt_attended, decode_attended)


def solution(mesh):
    finer = Mesh(
        mesh.devices.reshape(mesh.shape["rep"], 8, 16, mesh.shape["head"]),
        ("rep", "seq_0", "seq_1", "head"),
    )
    placed = (
        P(REP_SEQ_HEAD, None),
        P(REP_SEQ_HEAD, None),
        P(REP_SEQ_HEAD, None),
        P("rep"),
        P("rep"),
        P("rep", "head"),
        P("rep", "head"),
        P("rep", "head"),
        P("rep", "head", SEQ, None),
        P("rep", "head", SEQ, None),
        P("rep"),
    )
    return jax.shard_map(
        per_device,
        mesh=finer,
        in_specs=placed,
        out_specs=(P(REP_SEQ_HEAD, None), P("rep", "head")),
        check_vma=False,
    )
```

```python
import functools
import heapq
import math

import jax
import jax.numpy as jnp
import numpy as np
from jax import lax
from jax.experimental import pallas as pl
from jax.experimental.pallas import tpu as pltpu
from jax.sharding import Mesh
from jax.sharding import PartitionSpec as P

HD = 128
QH = 14
KVH = 2
GROUP = QH // KVH
SEQ = ("seq_0", "seq_1")
REP_SEQ_HEAD = ("rep", "seq_0", "seq_1", "head")
TILE = 8
NEG = -1e30
MESH = pl.DeviceIdType.MESH


def build_flow(n1, n2):
    half1, half2 = n1 // 2, n2 // 2
    members = {0: [0], half1: [-half1]}
    for k in range(1, half1):
        members[k] = [-k, k]
    heap, free, seq, arrived = [], {}, [0], {}
    order, first, sends = [], [], {}

    def send(now, link, item, into):
        units = len(members[item[2]]) if item[0] == 2 else 1
        begin = max(now, free.get(link, 0.0))
        free[link] = begin + units * (0.75 if link[0] == 2 else 1.4)
        seq[0] += 1
        heapq.heappush(heap, (free[link] + 2.5, seq[0], item))
        into.append(item)

    def phase2(now, k, into):
        for way in (1, -1):
            send(now, (2, way), (2, way, k, -way), into)

    for way in (1, -1):
        send(0.0, (1, way), (1, way, -way, 0), first)
    phase2(0.0, 0, first)
    groups = [(0, 0)]
    while heap:
        now, _, item = heapq.heappop(heap)
        order.append(item)
        into = sends.setdefault(item, [])
        ring, way, which, off2 = item
        if ring == 1:
            dist, k = abs(which), abs(which)
            if dist + 1 <= (half1 if way == 1 else half1 - 1):
                send(now, (1, way), (1, way, which - way, 0), into)
            arrived[k] = arrived.get(k, 0) + 1
            if arrived[k] == len(members[k]):
                groups.append((k, 0))
                phase2(now, k, into)
        else:
            dist = abs(off2)
            groups.append((which, off2))
            last = dist + 1 == half2 and way == (1 if which % 2 == 0 else -1)
            if dist + 1 < half2 or last:
                send(now, (2, way), (2, way, which, off2 - way), into)
    slot, offsets = {}, []
    for k, off2 in groups:
        slot[(k, off2)] = len(offsets)
        offsets.extend((m, off2) for m in members[k])

    def place(item):
        ring, _, which, off2 = item
        if ring == 2:
            return slot[(which, off2)], len(members[which])
        return slot[(abs(which), 0)] + members[abs(which)].index(which), 1

    number = {item: i for i, item in enumerate(order)}

    def resolve(items):
        out = []
        for item in items:
            ring, way, which, off2 = item
            source = (1, way, which + way, 0) if ring == 1 else (2, way, which, off2 + way)
            if ring == 1 and source[2] == 0:
                src = slot[(0, 0)]
            else:
                src = place(source)[0]
            dst, count = place(item)
            out.append((ring, way, src, dst, count, number[item]))
        return out

    steps, total = [], len(offsets) // TILE
    events = [(place(item), resolve(sends[item]), number[item]) for item in order]
    at, filled = 0, {0}
    for tile in range(total):
        need = set(range(tile * TILE, (tile + 1) * TILE))
        mine = []
        while not need <= filled:
            (dst, count), todo, sem = events[at]
            filled.update(range(dst, dst + count))
            mine.append((dst, count, todo, sem))
            at += 1
        steps.append(mine)
    assert at == len(events) and len(offsets) == n1 * n2
    return offsets, resolve(first), steps, len(events)


def attention_kernel(
    flows,
    sizes,
    span_ref,
    limit_ref,
    q_ref,
    bias_ref,
    k_ref,
    v_ref,
    len_ref,
    nq_ref,
    nk_ref,
    nv_ref,
    ck_ref,
    cv_ref,
    out_ref,
    dec_ref,
    buf,
    q_s,
    acc,
    top,
    tot,
    ck,
    cv,
    q_dec,
    p_dec,
    stat,
    part,
    got1,
    mine1,
    got2,
    mine2,
    got3,
    last,
    got4,
    local_sem,
    recv_sem,
    send_sem,
    pair_recv,
    pair_send,
    dec_recv,
    dec_send,
):
    n_x, n_z = sizes
    rows = q_ref.shape[0]
    x, z, core = lax.axis_index("seq_0"), lax.axis_index("seq_1"), lax.axis_index("head")
    steps = len(flows[0][2])
    names = ("seq_0", "seq_1")
    here = (x, z)
    extent = (n_x, n_z)

    def target(dim, way):
        return {names[dim]: lax.rem(here[dim] + way + extent[dim], extent[dim])}

    partner = {"head": 1 - core}
    in_k = pltpu.make_async_copy(k_ref, buf.at[0, 0, :, : KVH * HD], local_sem.at[0])
    in_v = pltpu.make_async_copy(v_ref, buf.at[0, 0, :, KVH * HD :], local_sem.at[1])
    in_k.start()
    in_v.start()
    in_ck = pltpu.make_async_copy(ck_ref.at[:, 0], ck, local_sem.at[2])
    in_cv = pltpu.make_async_copy(cv_ref.at[:, 0], cv, local_sem.at[3])
    in_ck.start()
    in_cv.start()
    barrier = pltpu.get_barrier_semaphore()
    for dim in (0, 1):
        for way in (1, -1):
            pl.semaphore_signal(barrier, inc=1, device_id=target(dim, way), device_id_type=MESH)
    pl.semaphore_signal(barrier, inc=1, device_id=partner, device_id_type=MESH)
    in_k.wait()
    in_v.wait()
    pl.semaphore_wait(barrier, 5)

    def ring_copy(flow, send):
        ring, way, src, dst, count, sem = send
        dim = (ring - 1) if flow == 0 else (2 - ring)
        return pltpu.make_async_remote_copy(
            src_ref=buf.at[0, pl.ds(src, count)],
            dst_ref=buf.at[0, pl.ds(dst, count)],
            send_sem=send_sem.at[0],
            recv_sem=recv_sem.at[sem],
            device_id=target(dim, way),
            device_id_type=MESH,
        )

    def pair_copy(tile):
        return pltpu.make_async_remote_copy(
            src_ref=buf.at[0, pl.ds(tile * TILE, TILE)],
            dst_ref=buf.at[1, pl.ds(tile * TILE, TILE)],
            send_sem=pair_send.at[0],
            recv_sem=pair_recv.at[tile],
            device_id=partner,
            device_id_type=MESH,
        )

    for flow in (0, 1):

        @pl.when(core == flow)
        def _():
            for send in flows[flow][1]:
                ring_copy(flow, send).start()

    scale = math.log2(math.e) / math.sqrt(HD)

    row = lax.broadcasted_iota(jnp.int32, (rows, rows), 0)
    col = lax.broadcasted_iota(jnp.int32, (rows, rows), 1)
    tri = jnp.concatenate([jnp.where(col <= row, 0.0, NEG).astype(jnp.float32)] * GROUP, axis=0)
    for g in range(KVH):
        for h in range(GROUP):
            head = g * GROUP + h
            q_s[g, h * rows : (h + 1) * rows, :] = q_ref[:, head * HD : (head + 1) * HD]
        key = buf[0, 0, :, g * HD : (g + 1) * HD]
        value = buf[0, 0, :, (KVH + g) * HD : (KVH + g + 1) * HD]
        s = lax.dot_general(q_s[g], key, (((1,), (1,)), ((), ())), preferred_element_type=jnp.float32)
        s = s + tri
        m = jnp.max(s, axis=1, keepdims=True)
        p = jnp.exp2((s - m) * scale)
        top[g] = jnp.broadcast_to(m, (GROUP * rows, HD))
        total = jnp.sum(p, axis=1, keepdims=True)
        lane = lax.broadcasted_iota(jnp.int32, (GROUP * rows, HD), 1)
        tot[g] = jnp.where(lane == 0, total, 0.0)
        acc[g] = jnp.dot(p.astype(jnp.bfloat16), value, preferred_element_type=jnp.float32)

    keys = TILE * rows

    def attend(side, tile):
        at = pl.ds(tile * TILE, TILE)
        bias = bias_ref[side * steps + tile]
        for g in range(KVH):
            key = buf[side, at, :, g * HD : (g + 1) * HD].reshape(keys, HD)
            value = buf[side, at, :, (KVH + g) * HD : (KVH + g + 1) * HD].reshape(keys, HD)
            s = lax.dot_general(
                q_s[g], key, (((1,), (1,)), ((), ())), preferred_element_type=jnp.float32
            )
            s = s + bias
            m_old = top[g]
            m = jnp.maximum(m_old, jnp.max(s, axis=1, keepdims=True))
            factor = jnp.exp2((m_old - m) * scale)
            m_wide = jnp.concatenate([m] * (keys // HD), axis=1)
            p = jnp.exp2((s - m_wide) * scale)
            part = p[:, :HD]
            for b in range(1, keys // HD):
                part = part + p[:, b * HD : (b + 1) * HD]
            top[g] = m
            tot[g] = tot[g] * factor + part
            acc[g] = acc[g] * factor + jnp.dot(
                p.astype(jnp.bfloat16), value, preferred_element_type=jnp.float32
            )

    sessions, ctx = ck_ref.shape[0], ck_ref.shape[2]
    tall = sessions * 8
    share = sessions // n_x
    quad = math.isqrt(n_z)
    first_chip = (x == 0) & (z == 0)
    at_row = lax.broadcasted_iota(jnp.int32, (sessions, 8, HD), 1)
    at_lane = lax.broadcasted_iota(jnp.int32, (sessions, 8, HD), 2)

    def spread(h):
        r = lax.broadcasted_iota(jnp.int32, (tall, sessions), 0)
        c = lax.broadcasted_iota(jnp.int32, (tall, sessions), 1)
        return jnp.where(r == c * 8 + h, 1.0, 0.0).astype(jnp.bfloat16)

    def pack(m, l, o):
        n = o.shape[0]
        row_n, lane_n = at_row[:n], at_lane[:n]
        line = jnp.where(lane_n == row_n, m, 0.0) + jnp.where(lane_n == row_n + 8, l, 0.0)
        line = jnp.sum(line, axis=1, keepdims=True)
        return jnp.where(row_n == 7, line, o)

    def combine(tiles):
        n = tiles[0].shape[0]
        row_n, lane_n = at_row[:n], at_lane[:n]
        tops, totals = [], []
        for t in tiles:
            line = jnp.broadcast_to(t[:, 7:8, :], t.shape)
            tops.append(jnp.sum(jnp.where(lane_n == row_n, line, 0.0), axis=2, keepdims=True))
            totals.append(jnp.sum(jnp.where(lane_n == row_n + 8, line, 0.0), axis=2, keepdims=True))
        m = functools.reduce(jnp.maximum, tops)
        l, o = 0.0, 0.0
        for t, t_top, t_total in zip(tiles, tops, totals):
            f = jnp.exp2((t_top - m) * scale)
            l = l + t_total * f
            o = o + t * f
        return m, l, o

    def decode_scores():
        q_all = 0.0
        for h in range(GROUP):
            q_all = q_all + jnp.dot(
                spread(h), nq_ref[:, h * HD : (h + 1) * HD], preferred_element_type=jnp.float32
            )
        q_dec[...] = q_all.reshape(sessions, 8, HD)
        in_ck.wait()
        begin = (x * n_z + z) * ctx
        spot = lax.broadcasted_iota(jnp.int32, (8, ctx), 1) + begin
        scores, valid, own = [], [], []
        for s_id in range(sessions):
            q_one = q_dec[s_id]
            scores.append(
                lax.dot_general(
                    q_one.astype(jnp.bfloat16),
                    ck[s_id],
                    (((1,), (1,)), ((), ())),
                    preferred_element_type=jnp.float32,
                )
            )
            valid.append(jnp.where(spot < len_ref[s_id], 0.0, NEG))
            own.append(q_one * nk_ref[s_id : s_id + 1, :].astype(jnp.float32))
        bar = jnp.concatenate(valid, axis=0)
        s = jnp.concatenate(scores, axis=0) + bar
        own = jnp.sum(jnp.concatenate(own, axis=0), axis=1, keepdims=True)
        own = jnp.where(first_chip, own, NEG)
        m = jnp.maximum(jnp.max(s, axis=1, keepdims=True), own)
        p = jnp.where(bar < 0.0, 0.0, jnp.exp2((s - m) * scale))
        p_own = jnp.where(first_chip, jnp.exp2((own - m) * scale), 0.0)
        total = jnp.sum(p, axis=1, keepdims=True) + p_own
        p_dec[...] = p.reshape(sessions, 8, ctx)
        stat[0] = jnp.broadcast_to(m, (tall, HD))
        stat[1] = jnp.broadcast_to(total, (tall, HD))
        stat[2] = jnp.broadcast_to(p_own, (tall, HD))

    def decode_values():
        in_cv.wait()
        outs = []
        for s_id in range(sessions):
            o = jnp.dot(
                p_dec[s_id].astype(jnp.bfloat16), cv[s_id], preferred_element_type=jnp.float32
            )
            extra = stat[2, s_id * 8 : (s_id + 1) * 8, :].astype(jnp.bfloat16).astype(jnp.float32)
            outs.append(o + extra * nv_ref[s_id : s_id + 1, :].astype(jnp.float32))
        o = jnp.concatenate(outs, axis=0).reshape(sessions, 8, HD)
        m = stat[0].reshape(sessions, 8, HD)
        total = stat[1].reshape(sessions, 8, HD)
        part[...] = pack(m, total, o).reshape(part.shape)

    def exchange(number, src, dst, sem, to):
        return pltpu.make_async_remote_copy(
            src_ref=src,
            dst_ref=dst,
            send_sem=dec_send.at[number],
            recv_sem=dec_recv.at[sem],
            device_id=to,
            device_id_type=MESH,
        )

    base2, base3, base4 = n_x, n_x + quad, n_x + 2 * quad

    def round1(d):
        to = lax.rem(x + d, n_x)
        return exchange(0, part.at[to], got1.at[d - 1], d, {"seq_0": to})

    def round2(d):
        to = (z // quad) * quad + lax.rem(lax.rem(z, quad) + d, quad)
        return exchange(1, mine1, got2.at[d - 1], base2 + d, {"seq_1": to})

    def round3(d):
        to = lax.rem(z + d * quad, n_z)
        return exchange(2, mine2, got3.at[d - 1], base3 + d, {"seq_1": to})

    def round4(d):
        to = lax.rem(x + d, n_x)
        return exchange(3, last, got4.at[d - 1], base4 + d, {"seq_0": to})

    def decode_round(j):
        @pl.when(j == 3)
        def _():
            for d in range(1, n_x):
                round1(d).start()

        @pl.when(j == 5)
        def _():
            for d in range(1, n_x):
                round1(d).wait_recv()
            mine1[...] = pack(*combine([part[x]] + [got1[d - 1] for d in range(1, n_x)]))

        @pl.when(j == 6)
        def _():
            for d in range(1, quad):
                round2(d).start()

        @pl.when(j == 8)
        def _():
            for d in range(1, quad):
                round2(d).wait_recv()
            mine2[...] = pack(*combine([mine1[...]] + [got2[d - 1] for d in range(1, quad)]))

        @pl.when(j == 10)
        def _():
            for d in range(1, quad):
                round3(d).start()

        @pl.when(j == 13)
        def _():
            for d in range(1, quad):
                round3(d).wait_recv()
            _, l, o = combine([mine2[...]] + [got3[d - 1] for d in range(1, quad)])
            last[...] = jnp.where(at_row[:share] == 7, 0.0, o / l)

        @pl.when(j == 14)
        def _():
            for d in range(1, n_x):
                round4(d).start()

    def receive(flow, arrivals):
        for dst, count, todo, sem in arrivals:
            pltpu.make_async_remote_copy(
                src_ref=buf.at[0, pl.ds(dst, count)],
                dst_ref=buf.at[0, pl.ds(dst, count)],
                send_sem=send_sem.at[0],
                recv_sem=recv_sem.at[sem],
                device_id=partner,
                device_id_type=MESH,
            ).wait_recv()
            for send in todo:
                ring_copy(flow, send).start()

    def step(j, carry):
        @pl.when(j == 0)
        def _():
            for lo, hi, work in ((0, 2, decode_scores), (2, 4, decode_values), (4, None, None)):
                for flow in (0, 1):

                    @pl.when(core == flow)
                    def _():
                        receive(flow, flows[flow][2][0][lo:hi])

                if work is not None:
                    work()

        for flow in (0, 1):
            for jj in range(1, steps):

                @pl.when((core == flow) & (j == jj))
                def _():
                    receive(flow, flows[flow][2][jj])

        decode_round(j)
        pair_copy(j).start()
        attend(0, j)

        @pl.when(j > 0)
        def _():
            pair_copy(j - 1).wait_recv()
            attend(1, j - 1)

        return carry

    lax.fori_loop(0, steps, step, 0)
    pair_copy(steps - 1).wait_recv()
    attend(1, steps - 1)

    for d in range(1, n_x):
        round4(d).wait_recv()
    got4[n_x - 1] = last[...]
    final = got4[...].reshape(tall, HD).astype(jnp.bfloat16)
    for h in range(GROUP):
        r = lax.broadcasted_iota(jnp.int32, (sessions, tall), 0)
        c = lax.broadcasted_iota(jnp.int32, (sessions, tall), 1)
        owner = lax.rem(x - 1 - c // (8 * share) + 2 * n_x, n_x)
        pick = (owner == r // share) & (lax.rem(c // 8, share) == lax.rem(r, share))
        pick = jnp.where(pick & (lax.rem(c, 8) == h), 1.0, 0.0).astype(jnp.bfloat16)
        row = jnp.dot(pick, final, preferred_element_type=jnp.float32)
        dec_ref[:, h * HD : (h + 1) * HD] = row.astype(jnp.bfloat16)

    def drain(number, ref):
        exchange(number, ref, ref, 0, partner).wait_send()

    drain(0, got1)
    drain(1, got2)
    drain(2, got3)
    drain(3, got4.at[pl.ds(0, n_x - 1)])
    chips = n_x * n_z
    pltpu.make_async_remote_copy(
        src_ref=buf.at[0, pl.ds(0, chips - 1)],
        dst_ref=buf.at[0, pl.ds(0, chips - 1)],
        send_sem=send_sem.at[0],
        recv_sem=recv_sem.at[0],
        device_id=partner,
        device_id_type=MESH,
    ).wait_send()
    pltpu.make_async_remote_copy(
        src_ref=buf.at[0, pl.ds(0, chips)],
        dst_ref=buf.at[1, pl.ds(0, chips)],
        send_sem=pair_send.at[0],
        recv_sem=recv_sem.at[0],
        device_id=partner,
        device_id_type=MESH,
    ).wait_send()

    me = (x * n_z + z) * 2 + core
    position = span_ref[me] * rows + lax.broadcasted_iota(jnp.int32, (rows, HD), 0)
    live = position < limit_ref[0]
    for g in range(KVH):
        for h in range(GROUP):
            head = g * GROUP + h
            at = slice(h * rows, (h + 1) * rows)
            total = jnp.sum(tot[g, at, :], axis=1, keepdims=True)
            result = jnp.where(live, acc[g, at, :] / total, 0.0)
            out_ref[:, head * HD : (head + 1) * HD] = result.astype(jnp.bfloat16)


def per_device(
    prompt_query,
    prompt_key,
    prompt_value,
    prompt_length,
    span_order,
    new_query,
    new_key,
    new_value,
    cache_key,
    cache_value,
    cache_length,
):
    rows = prompt_query.shape[0]
    n_x, n_z = lax.axis_size("seq_0"), lax.axis_size("seq_1")
    x, z, core = lax.axis_index("seq_0"), lax.axis_index("seq_1"), lax.axis_index("head")
    flow_a = build_flow(n_x, n_z)
    flow_b = build_flow(n_z, n_x)
    flows = (flow_a, flow_b)
    steps = len(flow_a[2])
    off = np.array(
        [[[a, b] for a, b in flow_a[0]], [[b, a] for a, b in flow_b[0]]], np.int32
    )
    order = jnp.where(core == 0, off, off[::-1])
    which = jnp.stack([core, 1 - core]).astype(jnp.int32)
    at_x = (order[..., 0] + x + n_x) % n_x
    at_z = (order[..., 1] + z + n_z) % n_z
    index = ((at_x * n_z + at_z) * 2 + which[:, None]).reshape(-1)
    me = (x * n_z + z) * 2 + core
    numbers = jnp.arange(span_order.shape[0], dtype=jnp.int32)
    picked = jnp.sum(jnp.where(index[:, None] == numbers[None, :], span_order[None, :], 0), axis=1)
    own = jnp.sum(jnp.where(me == numbers, span_order, 0))
    bias = jnp.where(picked < own, 0.0, NEG).astype(jnp.float32)
    bias = jnp.broadcast_to(bias[:, None], (bias.shape[0], rows)).reshape(2 * steps, 1, TILE * rows)
    width = 2 * KVH * HD
    sems = max(flow_a[3], flow_b[3])
    sessions, ctx = cache_key.shape[0], cache_key.shape[2]
    share, quad = sessions // n_x, math.isqrt(n_z)
    return pl.pallas_call(
        lambda *refs: attention_kernel(flows, (n_x, n_z), *refs),
        out_shape=(
            jax.ShapeDtypeStruct(prompt_query.shape, jnp.bfloat16),
            jax.ShapeDtypeStruct(new_query.shape, jnp.bfloat16),
        ),
        in_specs=[
            pl.BlockSpec(memory_space=pltpu.SMEM),
            pl.BlockSpec(memory_space=pltpu.SMEM),
            pl.BlockSpec(memory_space=pltpu.VMEM),
            pl.BlockSpec(memory_space=pltpu.VMEM),
            pl.BlockSpec(memory_space=pl.ANY),
            pl.BlockSpec(memory_space=pl.ANY),
            pl.BlockSpec(memory_space=pltpu.SMEM),
            pl.BlockSpec(memory_space=pltpu.VMEM),
            pl.BlockSpec(memory_space=pltpu.VMEM),
            pl.BlockSpec(memory_space=pltpu.VMEM),
            pl.BlockSpec(memory_space=pl.ANY),
            pl.BlockSpec(memory_space=pl.ANY),
        ],
        out_specs=(
            pl.BlockSpec(memory_space=pltpu.VMEM),
            pl.BlockSpec(memory_space=pltpu.VMEM),
        ),
        scratch_shapes=[
            pltpu.VMEM((2, n_x * n_z, rows, width), jnp.bfloat16),
            pltpu.VMEM((KVH, GROUP * rows, HD), jnp.bfloat16),
            pltpu.VMEM((KVH, GROUP * rows, HD), jnp.float32),
            pltpu.VMEM((KVH, GROUP * rows, HD), jnp.float32),
            pltpu.VMEM((KVH, GROUP * rows, HD), jnp.float32),
            pltpu.VMEM((sessions, ctx, HD), jnp.bfloat16),
            pltpu.VMEM((sessions, ctx, HD), jnp.bfloat16),
            pltpu.VMEM((sessions, 8, HD), jnp.float32),
            pltpu.VMEM((sessions, 8, ctx), jnp.float32),
            pltpu.VMEM((3, sessions * 8, HD), jnp.float32),
            pltpu.VMEM((n_x, share, 8, HD), jnp.float32),
            pltpu.VMEM((n_x - 1, share, 8, HD), jnp.float32),
            pltpu.VMEM((share, 8, HD), jnp.float32),
            pltpu.VMEM((quad - 1, share, 8, HD), jnp.float32),
            pltpu.VMEM((share, 8, HD), jnp.float32),
            pltpu.VMEM((quad - 1, share, 8, HD), jnp.float32),
            pltpu.VMEM((share, 8, HD), jnp.float32),
            pltpu.VMEM((n_x, share, 8, HD), jnp.float32),
            pltpu.SemaphoreType.DMA((4,)),
            pltpu.SemaphoreType.DMA((sems,)),
            pltpu.SemaphoreType.DMA((1,)),
            pltpu.SemaphoreType.DMA((steps,)),
            pltpu.SemaphoreType.DMA((1,)),
            pltpu.SemaphoreType.DMA((2 * n_x + 2 * quad,)),
            pltpu.SemaphoreType.DMA((4,)),
        ],
        compiler_params=pltpu.CompilerParams(
            collective_id=0, has_side_effects=True, vmem_limit_bytes=48 * 1024 * 1024
        ),
        name="prefill_decode_attention",
    )(
        span_order,
        prompt_length,
        prompt_query,
        bias,
        prompt_key,
        prompt_value,
        cache_length,
        new_query,
        new_key,
        new_value,
        cache_key,
        cache_value,
    )


def solution(mesh):
    finer = Mesh(
        mesh.devices.reshape(mesh.shape["rep"], 8, 16, mesh.shape["head"]),
        ("rep", "seq_0", "seq_1", "head"),
    )
    placed = (
        P(REP_SEQ_HEAD, None),
        P(REP_SEQ_HEAD, None),
        P(REP_SEQ_HEAD, None),
        P("rep"),
        P("rep"),
        P("rep", "head"),
        P("rep", "head"),
        P("rep", "head"),
        P("rep", "head", SEQ, None),
        P("rep", "head", SEQ, None),
        P("rep"),
    )
    return jax.shard_map(
        per_device,
        mesh=finer,
        in_specs=placed,
        out_specs=(P(REP_SEQ_HEAD, None), P("rep", "head")),
        check_vma=False,
    )
```

```python
import functools
import heapq
import math

import jax
import jax.numpy as jnp
import numpy as np
from jax import lax
from jax.experimental import pallas as pl
from jax.experimental.pallas import tpu as pltpu
from jax.sharding import Mesh
from jax.sharding import PartitionSpec as P

HD = 128
QH = 14
KVH = 2
GROUP = QH // KVH
SEQ = ("seq_0", "seq_1")
REP_SEQ_HEAD = ("rep", "seq_0", "seq_1", "head")
TILE = 8
NEG = -1e30
MESH = pl.DeviceIdType.MESH


def build_flow(n1, n2):
    half1, half2 = n1 // 2, n2 // 2
    members = {0: [0], half1: [-half1]}
    for k in range(1, half1):
        members[k] = [-k, k]
    heap, free, seq, arrived = [], {}, [0], {}
    order, first, sends = [], [], {}

    def send(now, link, item, into):
        units = len(members[item[2]]) if item[0] == 2 else 1
        begin = max(now, free.get(link, 0.0))
        free[link] = begin + units * (0.75 if link[0] == 2 else 1.4)
        seq[0] += 1
        heapq.heappush(heap, (free[link] + 2.5, seq[0], item))
        into.append(item)

    def phase2(now, k, into):
        for way in (1, -1):
            send(now, (2, way), (2, way, k, -way), into)

    for way in (1, -1):
        send(0.0, (1, way), (1, way, -way, 0), first)
    phase2(0.0, 0, first)
    groups = [(0, 0)]
    while heap:
        now, _, item = heapq.heappop(heap)
        order.append(item)
        into = sends.setdefault(item, [])
        ring, way, which, off2 = item
        if ring == 1:
            dist, k = abs(which), abs(which)
            if dist + 1 <= (half1 if way == 1 else half1 - 1):
                send(now, (1, way), (1, way, which - way, 0), into)
            arrived[k] = arrived.get(k, 0) + 1
            if arrived[k] == len(members[k]):
                groups.append((k, 0))
                phase2(now, k, into)
        else:
            dist = abs(off2)
            groups.append((which, off2))
            last = dist + 1 == half2 and way == (1 if which % 2 == 0 else -1)
            if dist + 1 < half2 or last:
                send(now, (2, way), (2, way, which, off2 - way), into)
    slot, offsets = {}, []
    for k, off2 in groups:
        slot[(k, off2)] = len(offsets)
        offsets.extend((m, off2) for m in members[k])

    def place(item):
        ring, _, which, off2 = item
        if ring == 2:
            return slot[(which, off2)], len(members[which])
        return slot[(abs(which), 0)] + members[abs(which)].index(which), 1

    number = {item: i for i, item in enumerate(order)}

    def resolve(items):
        out = []
        for item in items:
            ring, way, which, off2 = item
            source = (1, way, which + way, 0) if ring == 1 else (2, way, which, off2 + way)
            if ring == 1 and source[2] == 0:
                src = slot[(0, 0)]
            else:
                src = place(source)[0]
            dst, count = place(item)
            out.append((ring, way, src, dst, count, number[item]))
        return out

    steps, total = [], len(offsets) // TILE
    events = [(place(item), resolve(sends[item]), number[item]) for item in order]
    at, filled = 0, {0}
    for tile in range(total):
        need = set(range(tile * TILE, (tile + 1) * TILE))
        mine = []
        while not need <= filled:
            (dst, count), todo, sem = events[at]
            filled.update(range(dst, dst + count))
            mine.append((dst, count, todo, sem))
            at += 1
        steps.append(mine)
    assert at == len(events) and len(offsets) == n1 * n2
    return offsets, resolve(first), steps, len(events)


def attention_kernel(
    flows,
    sizes,
    span_ref,
    limit_ref,
    place_ref,
    q_hbm,
    k_ref,
    v_ref,
    len_ref,
    nq_hbm,
    nk_hbm,
    nv_hbm,
    ck_ref,
    cv_ref,
    out_ref,
    dec_ref,
    buf,
    q_ref,
    nq_ref,
    nk_ref,
    nv_ref,
    q_s,
    acc,
    top,
    tot,
    ck,
    cv,
    q_dec,
    p_dec,
    stat,
    part,
    got1,
    mine1,
    got2,
    mine2,
    got3,
    last,
    got4,
    local_sem,
    recv_sem,
    send_sem,
    pair_recv,
    pair_send,
    dec_recv,
    dec_send,
):
    n_x, n_z = sizes
    rows = q_ref.shape[0]
    x, z, core = lax.axis_index("seq_0"), lax.axis_index("seq_1"), lax.axis_index("head")
    steps = len(flows[0][2])
    names = ("seq_0", "seq_1")
    here = (x, z)
    extent = (n_x, n_z)

    def target(dim, way):
        return {names[dim]: lax.rem(here[dim] + way + extent[dim], extent[dim])}

    partner = {"head": 1 - core}
    in_k = pltpu.make_async_copy(k_ref, buf.at[0, 0, :, : KVH * HD], local_sem.at[0])
    in_v = pltpu.make_async_copy(v_ref, buf.at[0, 0, :, KVH * HD :], local_sem.at[1])
    in_k.start()
    in_v.start()
    in_ck = pltpu.make_async_copy(ck_ref.at[:, 0], ck, local_sem.at[2])
    in_cv = pltpu.make_async_copy(cv_ref.at[:, 0], cv, local_sem.at[3])
    in_q = pltpu.make_async_copy(q_hbm, q_ref, local_sem.at[4])
    in_new = [
        pltpu.make_async_copy(src, dst, local_sem.at[5 + i])
        for i, (src, dst) in enumerate(((nq_hbm, nq_ref), (nk_hbm, nk_ref), (nv_hbm, nv_ref)))
    ]
    in_q.start()
    in_ck.start()
    in_cv.start()
    for copy in in_new:
        copy.start()
    barrier = pltpu.get_barrier_semaphore()
    for dim in (0, 1):
        for way in (1, -1):
            pl.semaphore_signal(barrier, inc=1, device_id=target(dim, way), device_id_type=MESH)
    pl.semaphore_signal(barrier, inc=1, device_id=partner, device_id_type=MESH)
    in_k.wait()
    in_v.wait()
    pl.semaphore_wait(barrier, 5)

    def ring_copy(flow, send):
        ring, way, src, dst, count, sem = send
        dim = (ring - 1) if flow == 0 else (2 - ring)
        return pltpu.make_async_remote_copy(
            src_ref=buf.at[0, pl.ds(src, count)],
            dst_ref=buf.at[0, pl.ds(dst, count)],
            send_sem=send_sem.at[0],
            recv_sem=recv_sem.at[sem],
            device_id=target(dim, way),
            device_id_type=MESH,
        )

    def pair_copy(tile):
        return pltpu.make_async_remote_copy(
            src_ref=buf.at[0, pl.ds(tile * TILE, TILE)],
            dst_ref=buf.at[1, pl.ds(tile * TILE, TILE)],
            send_sem=pair_send.at[0],
            recv_sem=pair_recv.at[tile],
            device_id=partner,
            device_id_type=MESH,
        )

    for flow in (0, 1):

        @pl.when(core == flow)
        def _():
            for send in flows[flow][1]:
                ring_copy(flow, send).start()

    scale = math.log2(math.e) / math.sqrt(HD)

    in_q.wait()
    row = lax.broadcasted_iota(jnp.int32, (rows, rows), 0)
    col = lax.broadcasted_iota(jnp.int32, (rows, rows), 1)
    tri = jnp.concatenate([jnp.where(col <= row, 0.0, NEG).astype(jnp.float32)] * GROUP, axis=0)
    for g in range(KVH):
        for h in range(GROUP):
            head = g * GROUP + h
            q_s[g, h * rows : (h + 1) * rows, :] = q_ref[:, head * HD : (head + 1) * HD]
        key = buf[0, 0, :, g * HD : (g + 1) * HD]
        value = buf[0, 0, :, (KVH + g) * HD : (KVH + g + 1) * HD]
        s = lax.dot_general(q_s[g], key, (((1,), (1,)), ((), ())), preferred_element_type=jnp.float32)
        s = s + tri
        m = jnp.max(s, axis=1, keepdims=True)
        p = jnp.exp2((s - m) * scale)
        top[g] = jnp.broadcast_to(m, (GROUP * rows, HD))
        total = jnp.sum(p, axis=1, keepdims=True)
        lane = lax.broadcasted_iota(jnp.int32, (GROUP * rows, HD), 1)
        tot[g] = jnp.where(lane == 0, total, 0.0)
        acc[g] = jnp.dot(p.astype(jnp.bfloat16), value, preferred_element_type=jnp.float32)

    keys = TILE * rows
    own_span = span_ref[(x * n_z + z) * 2 + core]

    def attend(side, tile):
        at = pl.ds(tile * TILE, TILE)
        flow = core if side == 0 else 1 - core
        marks = []
        for b in range(TILE):
            slot = flow * n_x * n_z + tile * TILE + b
            at_x = lax.rem(x + place_ref[slot], n_x)
            at_z = lax.rem(z + place_ref[2 * n_x * n_z + slot], n_z)
            span = span_ref[(at_x * n_z + at_z) * 2 + flow]
            marks.append(jnp.where(span < own_span, 0.0, NEG).astype(jnp.float32))
        lane = lax.broadcasted_iota(jnp.int32, (1, HD), 1)
        bias = []
        for b in range(0, TILE, 2):
            bias.append(jnp.where(lane < rows, marks[b], marks[b + 1]))
        bias = jnp.concatenate(bias, axis=1)
        for g in range(KVH):
            key = buf[side, at, :, g * HD : (g + 1) * HD].reshape(keys, HD)
            value = buf[side, at, :, (KVH + g) * HD : (KVH + g + 1) * HD].reshape(keys, HD)
            s = lax.dot_general(
                q_s[g], key, (((1,), (1,)), ((), ())), preferred_element_type=jnp.float32
            )
            s = s + bias
            m_old = top[g]
            m = jnp.maximum(m_old, jnp.max(s, axis=1, keepdims=True))
            factor = jnp.exp2((m_old - m) * scale)
            m_wide = jnp.concatenate([m] * (keys // HD), axis=1)
            p = jnp.exp2((s - m_wide) * scale)
            part = p[:, :HD]
            for b in range(1, keys // HD):
                part = part + p[:, b * HD : (b + 1) * HD]
            top[g] = m
            tot[g] = tot[g] * factor + part
            acc[g] = acc[g] * factor + jnp.dot(
                p.astype(jnp.bfloat16), value, preferred_element_type=jnp.float32
            )

    sessions, ctx = ck_ref.shape[0], ck_ref.shape[2]
    tall = sessions * 8
    share = sessions // n_x
    quad = math.isqrt(n_z)
    first_chip = (x == 0) & (z == 0)
    at_row = lax.broadcasted_iota(jnp.int32, (sessions, 8, HD), 1)
    at_lane = lax.broadcasted_iota(jnp.int32, (sessions, 8, HD), 2)

    def spread(h):
        r = lax.broadcasted_iota(jnp.int32, (tall, sessions), 0)
        c = lax.broadcasted_iota(jnp.int32, (tall, sessions), 1)
        return jnp.where(r == c * 8 + h, 1.0, 0.0).astype(jnp.bfloat16)

    def pack(m, l, o):
        n = o.shape[0]
        row_n, lane_n = at_row[:n], at_lane[:n]
        line = jnp.where(lane_n == row_n, m, 0.0) + jnp.where(lane_n == row_n + 8, l, 0.0)
        line = jnp.sum(line, axis=1, keepdims=True)
        return jnp.where(row_n == 7, line, o)

    def combine(tiles):
        n = tiles[0].shape[0]
        row_n, lane_n = at_row[:n], at_lane[:n]
        tops, totals = [], []
        for t in tiles:
            line = jnp.broadcast_to(t[:, 7:8, :], t.shape)
            tops.append(jnp.sum(jnp.where(lane_n == row_n, line, 0.0), axis=2, keepdims=True))
            totals.append(jnp.sum(jnp.where(lane_n == row_n + 8, line, 0.0), axis=2, keepdims=True))
        m = functools.reduce(jnp.maximum, tops)
        l, o = 0.0, 0.0
        for t, t_top, t_total in zip(tiles, tops, totals):
            f = jnp.exp2((t_top - m) * scale)
            l = l + t_total * f
            o = o + t * f
        return m, l, o

    def decode_scores():
        for copy in in_new:
            copy.wait()
        q_all = 0.0
        for h in range(GROUP):
            q_all = q_all + jnp.dot(
                spread(h), nq_ref[:, h * HD : (h + 1) * HD], preferred_element_type=jnp.float32
            )
        q_dec[...] = q_all.reshape(sessions, 8, HD)
        in_ck.wait()
        begin = (x * n_z + z) * ctx
        spot = lax.broadcasted_iota(jnp.int32, (8, ctx), 1) + begin
        scores, valid, own = [], [], []
        for s_id in range(sessions):
            q_one = q_dec[s_id]
            scores.append(
                lax.dot_general(
                    q_one.astype(jnp.bfloat16),
                    ck[s_id],
                    (((1,), (1,)), ((), ())),
                    preferred_element_type=jnp.float32,
                )
            )
            valid.append(jnp.where(spot < len_ref[s_id], 0.0, NEG))
            own.append(q_one * nk_ref[s_id : s_id + 1, :].astype(jnp.float32))
        bar = jnp.concatenate(valid, axis=0)
        s = jnp.concatenate(scores, axis=0) + bar
        own = jnp.sum(jnp.concatenate(own, axis=0), axis=1, keepdims=True)
        own = jnp.where(first_chip, own, NEG)
        m = jnp.maximum(jnp.max(s, axis=1, keepdims=True), own)
        p = jnp.where(bar < 0.0, 0.0, jnp.exp2((s - m) * scale))
        p_own = jnp.where(first_chip, jnp.exp2((own - m) * scale), 0.0)
        total = jnp.sum(p, axis=1, keepdims=True) + p_own
        p_dec[...] = p.reshape(sessions, 8, ctx)
        stat[0] = jnp.broadcast_to(m, (tall, HD))
        stat[1] = jnp.broadcast_to(total, (tall, HD))
        stat[2] = jnp.broadcast_to(p_own, (tall, HD))

    def decode_values():
        in_cv.wait()
        outs = []
        for s_id in range(sessions):
            o = jnp.dot(
                p_dec[s_id].astype(jnp.bfloat16), cv[s_id], preferred_element_type=jnp.float32
            )
            extra = stat[2, s_id * 8 : (s_id + 1) * 8, :].astype(jnp.bfloat16).astype(jnp.float32)
            outs.append(o + extra * nv_ref[s_id : s_id + 1, :].astype(jnp.float32))
        o = jnp.concatenate(outs, axis=0).reshape(sessions, 8, HD)
        m = stat[0].reshape(sessions, 8, HD)
        total = stat[1].reshape(sessions, 8, HD)
        part[...] = pack(m, total, o).reshape(part.shape)

    def exchange(number, src, dst, sem, to):
        return pltpu.make_async_remote_copy(
            src_ref=src,
            dst_ref=dst,
            send_sem=dec_send.at[number],
            recv_sem=dec_recv.at[sem],
            device_id=to,
            device_id_type=MESH,
        )

    base2, base3, base4 = n_x, n_x + quad, n_x + 2 * quad

    def round1(d):
        to = lax.rem(x + d, n_x)
        return exchange(0, part.at[to], got1.at[d - 1], d, {"seq_0": to})

    def round2(d):
        to = (z // quad) * quad + lax.rem(lax.rem(z, quad) + d, quad)
        return exchange(1, mine1, got2.at[d - 1], base2 + d, {"seq_1": to})

    def round3(d):
        to = lax.rem(z + d * quad, n_z)
        return exchange(2, mine2, got3.at[d - 1], base3 + d, {"seq_1": to})

    def round4(d):
        to = lax.rem(x + d, n_x)
        return exchange(3, last, got4.at[d - 1], base4 + d, {"seq_0": to})

    def decode_round(j):
        @pl.when(j == 5)
        def _():
            decode_scores()

        @pl.when(j == 6)
        def _():
            decode_values()

        @pl.when(j == 8)
        def _():
            for d in range(1, n_x):
                round1(d).wait_recv()
            mine1[...] = pack(*combine([part[x]] + [got1[d - 1] for d in range(1, n_x)]))

        @pl.when(j == 10)
        def _():
            for d in range(1, quad):
                round2(d).wait_recv()
            mine2[...] = pack(*combine([mine1[...]] + [got2[d - 1] for d in range(1, quad)]))

        @pl.when(j == 13)
        def _():
            for d in range(1, quad):
                round3(d).wait_recv()
            _, l, o = combine([mine2[...]] + [got3[d - 1] for d in range(1, quad)])
            last[...] = jnp.where(at_row[:share] == 7, 0.0, o / l)

    def decode_send(j):
        for at, one_round, count in ((6, round1, n_x), (8, round2, quad), (10, round3, quad), (13, round4, n_x)):

            @pl.when(j == at)
            def _():
                for d in range(1, count):
                    one_round(d).start()

    def receive(flow, arrivals):
        for dst, count, todo, sem in arrivals:
            pltpu.make_async_remote_copy(
                src_ref=buf.at[0, pl.ds(dst, count)],
                dst_ref=buf.at[0, pl.ds(dst, count)],
                send_sem=send_sem.at[0],
                recv_sem=recv_sem.at[sem],
                device_id=partner,
                device_id_type=MESH,
            ).wait_recv()
            for send in todo:
                ring_copy(flow, send).start()

    def step(j, carry):
        for flow in (0, 1):
            for jj in range(steps):

                @pl.when((core == flow) & (j == jj))
                def _():
                    receive(flow, flows[flow][2][jj])

        decode_round(j)
        pair_copy(j).start()
        attend(0, j)

        @pl.when(j > 0)
        def _():
            pair_copy(j - 1).wait_recv()
            attend(1, j - 1)

        decode_send(j)
        return carry

    lax.fori_loop(0, steps, step, 0)
    pair_copy(steps - 1).wait_recv()
    attend(1, steps - 1)

    for d in range(1, n_x):
        round4(d).wait_recv()
    got4[n_x - 1] = last[...]
    final = got4[...].reshape(tall, HD).astype(jnp.bfloat16)
    for h in range(GROUP):
        r = lax.broadcasted_iota(jnp.int32, (sessions, tall), 0)
        c = lax.broadcasted_iota(jnp.int32, (sessions, tall), 1)
        owner = lax.rem(x - 1 - c // (8 * share) + 2 * n_x, n_x)
        pick = (owner == r // share) & (lax.rem(c // 8, share) == lax.rem(r, share))
        pick = jnp.where(pick & (lax.rem(c, 8) == h), 1.0, 0.0).astype(jnp.bfloat16)
        row = jnp.dot(pick, final, preferred_element_type=jnp.float32)
        dec_ref[:, h * HD : (h + 1) * HD] = row.astype(jnp.bfloat16)

    def drain(number, ref):
        exchange(number, ref, ref, 0, partner).wait_send()

    drain(0, got1)
    drain(1, got2)
    drain(2, got3)
    drain(3, got4.at[pl.ds(0, n_x - 1)])
    chips = n_x * n_z
    pltpu.make_async_remote_copy(
        src_ref=buf.at[0, pl.ds(0, chips - 1)],
        dst_ref=buf.at[0, pl.ds(0, chips - 1)],
        send_sem=send_sem.at[0],
        recv_sem=recv_sem.at[0],
        device_id=partner,
        device_id_type=MESH,
    ).wait_send()
    pltpu.make_async_remote_copy(
        src_ref=buf.at[0, pl.ds(0, chips)],
        dst_ref=buf.at[1, pl.ds(0, chips)],
        send_sem=pair_send.at[0],
        recv_sem=recv_sem.at[0],
        device_id=partner,
        device_id_type=MESH,
    ).wait_send()

    me = (x * n_z + z) * 2 + core
    position = span_ref[me] * rows + lax.broadcasted_iota(jnp.int32, (rows, HD), 0)
    live = position < limit_ref[0]
    for g in range(KVH):
        for h in range(GROUP):
            head = g * GROUP + h
            at = slice(h * rows, (h + 1) * rows)
            total = jnp.sum(tot[g, at, :], axis=1, keepdims=True)
            result = jnp.where(live, acc[g, at, :] / total, 0.0)
            out_ref[:, head * HD : (head + 1) * HD] = result.astype(jnp.bfloat16)


def per_device(
    prompt_query,
    prompt_key,
    prompt_value,
    prompt_length,
    span_order,
    new_query,
    new_key,
    new_value,
    cache_key,
    cache_value,
    cache_length,
):
    rows = prompt_query.shape[0]
    n_x, n_z = lax.axis_size("seq_0"), lax.axis_size("seq_1")
    flow_a = build_flow(n_x, n_z)
    flow_b = build_flow(n_z, n_x)
    flows = (flow_a, flow_b)
    steps = len(flow_a[2])
    place_x = [a % n_x for a, _ in flow_a[0]] + [b % n_x for _, b in flow_b[0]]
    place_z = [b % n_z for _, b in flow_a[0]] + [a % n_z for a, _ in flow_b[0]]
    places = jnp.asarray(np.array(place_x + place_z, np.int32))
    width = 2 * KVH * HD
    sems = max(flow_a[3], flow_b[3])
    sessions, ctx = cache_key.shape[0], cache_key.shape[2]
    share, quad = sessions // n_x, math.isqrt(n_z)
    return pl.pallas_call(
        lambda *refs: attention_kernel(flows, (n_x, n_z), *refs),
        out_shape=(
            jax.ShapeDtypeStruct(prompt_query.shape, jnp.bfloat16),
            jax.ShapeDtypeStruct(new_query.shape, jnp.bfloat16),
        ),
        in_specs=[pl.BlockSpec(memory_space=pltpu.SMEM)] * 3
        + [pl.BlockSpec(memory_space=pltpu.HBM)] * 3
        + [pl.BlockSpec(memory_space=pltpu.SMEM)]
        + [pl.BlockSpec(memory_space=pltpu.HBM)] * 5,
        out_specs=(
            pl.BlockSpec(memory_space=pltpu.VMEM),
            pl.BlockSpec(memory_space=pltpu.VMEM),
        ),
        scratch_shapes=[
            pltpu.VMEM((2, n_x * n_z, rows, width), jnp.bfloat16),
            pltpu.VMEM(prompt_query.shape, jnp.bfloat16),
            pltpu.VMEM(new_query.shape, jnp.bfloat16),
            pltpu.VMEM(new_key.shape, jnp.bfloat16),
            pltpu.VMEM(new_value.shape, jnp.bfloat16),
            pltpu.VMEM((KVH, GROUP * rows, HD), jnp.bfloat16),
            pltpu.VMEM((KVH, GROUP * rows, HD), jnp.float32),
            pltpu.VMEM((KVH, GROUP * rows, HD), jnp.float32),
            pltpu.VMEM((KVH, GROUP * rows, HD), jnp.float32),
            pltpu.VMEM((sessions, ctx, HD), jnp.bfloat16),
            pltpu.VMEM((sessions, ctx, HD), jnp.bfloat16),
            pltpu.VMEM((sessions, 8, HD), jnp.float32),
            pltpu.VMEM((sessions, 8, ctx), jnp.float32),
            pltpu.VMEM((3, sessions * 8, HD), jnp.float32),
            pltpu.VMEM((n_x, share, 8, HD), jnp.float32),
            pltpu.VMEM((n_x - 1, share, 8, HD), jnp.float32),
            pltpu.VMEM((share, 8, HD), jnp.float32),
            pltpu.VMEM((quad - 1, share, 8, HD), jnp.float32),
            pltpu.VMEM((share, 8, HD), jnp.float32),
            pltpu.VMEM((quad - 1, share, 8, HD), jnp.float32),
            pltpu.VMEM((share, 8, HD), jnp.float32),
            pltpu.VMEM((n_x, share, 8, HD), jnp.float32),
            pltpu.SemaphoreType.DMA((8,)),
            pltpu.SemaphoreType.DMA((sems,)),
            pltpu.SemaphoreType.DMA((1,)),
            pltpu.SemaphoreType.DMA((steps,)),
            pltpu.SemaphoreType.DMA((1,)),
            pltpu.SemaphoreType.DMA((2 * n_x + 2 * quad,)),
            pltpu.SemaphoreType.DMA((4,)),
        ],
        compiler_params=pltpu.CompilerParams(
            collective_id=0, has_side_effects=True, vmem_limit_bytes=67_000_000
        ),
        name="prefill_decode_attention",
    )(
        span_order,
        prompt_length,
        places,
        prompt_query,
        prompt_key,
        prompt_value,
        cache_length,
        new_query,
        new_key,
        new_value,
        cache_key,
        cache_value,
    )


def solution(mesh):
    finer = Mesh(
        mesh.devices.reshape(mesh.shape["rep"], 8, 16, mesh.shape["head"]),
        ("rep", "seq_0", "seq_1", "head"),
    )
    placed = (
        P(REP_SEQ_HEAD, None),
        P(REP_SEQ_HEAD, None),
        P(REP_SEQ_HEAD, None),
        P("rep"),
        P("rep"),
        P("rep", "head"),
        P("rep", "head"),
        P("rep", "head"),
        P("rep", "head", SEQ, None),
        P("rep", "head", SEQ, None),
        P("rep"),
    )
    return jax.shard_map(
        per_device,
        mesh=finer,
        in_specs=placed,
        out_specs=(P(REP_SEQ_HEAD, None), P("rep", "head")),
        check_vma=False,
    )
```

```python
import functools
import heapq
import math

import jax
import jax.numpy as jnp
import numpy as np
from jax import lax
from jax.experimental import pallas as pl
from jax.experimental.pallas import tpu as pltpu
from jax.sharding import Mesh
from jax.sharding import PartitionSpec as P

HD = 128
QH = 14
KVH = 2
GROUP = QH // KVH
SEQ = ("seq_0", "seq_1")
REP_SEQ_HEAD = ("rep", "seq_0", "seq_1", "head")
TILE = 8
NEG = -1e30
MESH = pl.DeviceIdType.MESH


def build_flow(n1, n2):
    half1, half2 = n1 // 2, n2 // 2
    members = {0: [0], half1: [-half1]}
    for k in range(1, half1):
        members[k] = [-k, k]
    heap, free, seq, arrived = [], {}, [0], {}
    order, first, sends = [], [], {}

    def send(now, link, item, into):
        units = len(members[item[2]]) if item[0] == 2 else 1
        begin = max(now, free.get(link, 0.0))
        free[link] = begin + units * (0.75 if link[0] == 2 else 1.4)
        seq[0] += 1
        heapq.heappush(heap, (free[link] + 4.0, seq[0], item))
        into.append(item)

    def phase2(now, k, into):
        for way in (1, -1):
            send(now, (2, way), (2, way, k, -way), into)

    for way in (1, -1):
        send(0.0, (1, way), (1, way, -way, 0), first)
    phase2(0.0, 0, first)
    groups = [(0, 0)]
    while heap:
        now, _, item = heapq.heappop(heap)
        order.append(item)
        into = sends.setdefault(item, [])
        ring, way, which, off2 = item
        if ring == 1:
            dist, k = abs(which), abs(which)
            if dist + 1 <= (half1 if way == 1 else half1 - 1):
                send(now, (1, way), (1, way, which - way, 0), into)
            arrived[k] = arrived.get(k, 0) + 1
            if arrived[k] == len(members[k]):
                groups.append((k, 0))
                phase2(now, k, into)
        else:
            dist = abs(off2)
            groups.append((which, off2))
            last = dist + 1 == half2 and way == (1 if which % 2 == 0 else -1)
            if dist + 1 < half2 or last:
                send(now, (2, way), (2, way, which, off2 - way), into)
    slot, offsets = {}, []
    for k, off2 in groups:
        slot[(k, off2)] = len(offsets)
        offsets.extend((m, off2) for m in members[k])

    def place(item):
        ring, _, which, off2 = item
        if ring == 2:
            return slot[(which, off2)], len(members[which])
        return slot[(abs(which), 0)] + members[abs(which)].index(which), 1

    number = {item: i for i, item in enumerate(order)}

    def resolve(items):
        out = []
        for item in items:
            ring, way, which, off2 = item
            source = (1, way, which + way, 0) if ring == 1 else (2, way, which, off2 + way)
            if ring == 1 and source[2] == 0:
                src = slot[(0, 0)]
            else:
                src = place(source)[0]
            dst, count = place(item)
            out.append((ring, way, src, dst, count, number[item]))
        return out

    steps, total = [], 2 * len(offsets) // TILE
    events = [(place(item), resolve(sends[item]), number[item]) for item in order]
    at, filled = 0, {0}
    for half in range(total):
        need = set(range(half * TILE // 2, (half + 1) * TILE // 2))
        mine = []
        while not need <= filled:
            (dst, count), todo, sem = events[at]
            filled.update(range(dst, dst + count))
            mine.append((dst, count, todo, sem))
            at += 1
        steps.append(mine)
    assert at == len(events) and len(offsets) == n1 * n2
    return offsets, resolve(first), steps, len(events)


def attention_kernel(
    flows,
    sizes,
    span_hbm,
    limit_ref,
    place_hbm,
    q_hbm,
    k_ref,
    v_ref,
    len_hbm,
    nq_hbm,
    nk_hbm,
    nv_hbm,
    ck_ref,
    cv_ref,
    out_ref,
    dec_ref,
    buf,
    span_ref,
    place_ref,
    len_ref,
    q_ref,
    nq_ref,
    nk_ref,
    nv_ref,
    q_s,
    acc,
    top,
    tot,
    ck,
    cv,
    q_dec,
    p_dec,
    stat,
    part,
    got1,
    mine1,
    got2,
    mine2,
    got3,
    last,
    got4,
    local_sem,
    recv_sem,
    send_sem,
    pair_recv,
    pair_send,
    dec_recv,
    dec_send,
):
    n_x, n_z = sizes
    rows = q_ref.shape[0]
    x, z, core = lax.axis_index("seq_0"), lax.axis_index("seq_1"), lax.axis_index("head")
    steps = len(flows[0][2]) // 2
    names = ("seq_0", "seq_1")
    here = (x, z)
    extent = (n_x, n_z)

    def target(dim, way):
        return {names[dim]: lax.rem(here[dim] + way + extent[dim], extent[dim])}

    partner = {"head": 1 - core}
    barrier = pltpu.get_barrier_semaphore()
    for dim in (0, 1):
        for way in (1, -1):
            pl.semaphore_signal(barrier, inc=1, device_id=target(dim, way), device_id_type=MESH)
    pl.semaphore_signal(barrier, inc=1, device_id=partner, device_id_type=MESH)
    in_k = pltpu.make_async_copy(k_ref, buf.at[0, 0, :, : KVH * HD], local_sem.at[0])
    in_v = pltpu.make_async_copy(v_ref, buf.at[0, 0, :, KVH * HD :], local_sem.at[1])
    in_k.start()
    in_v.start()
    in_ck = pltpu.make_async_copy(ck_ref.at[:, 0], ck, local_sem.at[2])
    in_cv = pltpu.make_async_copy(cv_ref.at[:, 0], cv, local_sem.at[3])
    in_q = pltpu.make_async_copy(q_hbm, q_ref, local_sem.at[4])
    in_new = [
        pltpu.make_async_copy(src, dst, local_sem.at[5 + i])
        for i, (src, dst) in enumerate(((nq_hbm, nq_ref), (nk_hbm, nk_ref), (nv_hbm, nv_ref)))
    ]
    in_scalars = [
        pltpu.make_async_copy(src, dst, local_sem.at[8 + i])
        for i, (src, dst) in enumerate(
            ((span_hbm, span_ref), (place_hbm, place_ref), (len_hbm, len_ref))
        )
    ]
    in_q.start()
    for copy in in_scalars:
        copy.start()
    in_ck.start()
    in_cv.start()
    for copy in in_new:
        copy.start()
    in_k.wait()
    in_v.wait()
    pl.semaphore_wait(barrier, 5)

    def ring_copy(flow, send):
        ring, way, src, dst, count, sem = send
        dim = (ring - 1) if flow == 0 else (2 - ring)
        return pltpu.make_async_remote_copy(
            src_ref=buf.at[0, pl.ds(src, count)],
            dst_ref=buf.at[0, pl.ds(dst, count)],
            send_sem=send_sem.at[0],
            recv_sem=recv_sem.at[sem],
            device_id=target(dim, way),
            device_id_type=MESH,
        )

    def pair_copy(half):
        at = pl.ds(half * (TILE // 2), TILE // 2)
        return pltpu.make_async_remote_copy(
            src_ref=buf.at[0, at],
            dst_ref=buf.at[1, at],
            send_sem=pair_send.at[0],
            recv_sem=pair_recv.at[half],
            device_id=partner,
            device_id_type=MESH,
        )

    for flow in (0, 1):

        @pl.when(core == flow)
        def _():
            for send in flows[flow][1]:
                ring_copy(flow, send).start()

    scale = math.log2(math.e) / math.sqrt(HD)

    in_q.wait()
    row = lax.broadcasted_iota(jnp.int32, (rows, rows), 0)
    col = lax.broadcasted_iota(jnp.int32, (rows, rows), 1)
    tri = jnp.concatenate([jnp.where(col <= row, 0.0, NEG).astype(jnp.float32)] * GROUP, axis=0)
    for g in range(KVH):
        for h in range(GROUP):
            head = g * GROUP + h
            q_s[g, h * rows : (h + 1) * rows, :] = q_ref[:, head * HD : (head + 1) * HD]
        key = buf[0, 0, :, g * HD : (g + 1) * HD]
        value = buf[0, 0, :, (KVH + g) * HD : (KVH + g + 1) * HD]
        s = lax.dot_general(q_s[g], key, (((1,), (1,)), ((), ())), preferred_element_type=jnp.float32)
        s = s + tri
        m = jnp.max(s, axis=1, keepdims=True)
        p = jnp.exp2((s - m) * scale)
        top[g] = jnp.broadcast_to(m, (GROUP * rows, HD))
        total = jnp.sum(p, axis=1, keepdims=True)
        lane = lax.broadcasted_iota(jnp.int32, (GROUP * rows, HD), 1)
        tot[g] = jnp.where(lane == 0, total, 0.0)
        acc[g] = jnp.dot(p.astype(jnp.bfloat16), value, preferred_element_type=jnp.float32)

    keys = TILE * rows
    for copy in in_scalars:
        copy.wait()
    own_span = span_ref[(x * n_z + z) * 2 + core]

    def attend(side, tile):
        at = pl.ds(tile * TILE, TILE)
        flow = core if side == 0 else 1 - core
        marks = []
        for b in range(TILE):
            slot = flow * n_x * n_z + tile * TILE + b
            at_x = lax.rem(x + place_ref[slot], n_x)
            at_z = lax.rem(z + place_ref[2 * n_x * n_z + slot], n_z)
            span = span_ref[(at_x * n_z + at_z) * 2 + flow]
            marks.append(jnp.where(span < own_span, 0.0, NEG).astype(jnp.float32))
        lane = lax.broadcasted_iota(jnp.int32, (1, HD), 1)
        bias = []
        for b in range(0, TILE, 2):
            bias.append(jnp.where(lane < rows, marks[b], marks[b + 1]))
        bias = jnp.concatenate(bias, axis=1)
        for g in range(KVH):
            key = buf[side, at, :, g * HD : (g + 1) * HD].reshape(keys, HD)
            value = buf[side, at, :, (KVH + g) * HD : (KVH + g + 1) * HD].reshape(keys, HD)
            s = lax.dot_general(
                q_s[g], key, (((1,), (1,)), ((), ())), preferred_element_type=jnp.float32
            )
            s = s + bias
            m_old = top[g]
            m = jnp.maximum(m_old, jnp.max(s, axis=1, keepdims=True))
            factor = jnp.exp2((m_old - m) * scale)
            m_wide = jnp.concatenate([m] * (keys // HD), axis=1)
            p = jnp.exp2((s - m_wide) * scale)
            part = p[:, :HD]
            for b in range(1, keys // HD):
                part = part + p[:, b * HD : (b + 1) * HD]
            top[g] = m
            tot[g] = tot[g] * factor + part
            acc[g] = acc[g] * factor + jnp.dot(
                p.astype(jnp.bfloat16), value, preferred_element_type=jnp.float32
            )

    sessions, ctx = ck_ref.shape[0], ck_ref.shape[2]
    tall = sessions * 8
    share = sessions // n_x
    quad = math.isqrt(n_z)
    first_chip = (x == 0) & (z == 0)
    at_row = lax.broadcasted_iota(jnp.int32, (sessions, 8, HD), 1)
    at_lane = lax.broadcasted_iota(jnp.int32, (sessions, 8, HD), 2)

    def spread(h):
        r = lax.broadcasted_iota(jnp.int32, (tall, sessions), 0)
        c = lax.broadcasted_iota(jnp.int32, (tall, sessions), 1)
        return jnp.where(r == c * 8 + h, 1.0, 0.0).astype(jnp.bfloat16)

    def pack(m, l, o):
        n = o.shape[0]
        row_n, lane_n = at_row[:n], at_lane[:n]
        line = jnp.where(lane_n == row_n, m, 0.0) + jnp.where(lane_n == row_n + 8, l, 0.0)
        line = jnp.sum(line, axis=1, keepdims=True)
        return jnp.where(row_n == 7, line, o)

    def combine(tiles):
        n = tiles[0].shape[0]
        row_n, lane_n = at_row[:n], at_lane[:n]
        tops, totals = [], []
        for t in tiles:
            line = jnp.broadcast_to(t[:, 7:8, :], t.shape)
            tops.append(jnp.sum(jnp.where(lane_n == row_n, line, 0.0), axis=2, keepdims=True))
            totals.append(jnp.sum(jnp.where(lane_n == row_n + 8, line, 0.0), axis=2, keepdims=True))
        m = functools.reduce(jnp.maximum, tops)
        l, o = 0.0, 0.0
        for t, t_top, t_total in zip(tiles, tops, totals):
            f = jnp.exp2((t_top - m) * scale)
            l = l + t_total * f
            o = o + t * f
        return m, l, o

    def decode_scores():
        for copy in in_new:
            copy.wait()
        q_all = 0.0
        for h in range(GROUP):
            q_all = q_all + jnp.dot(
                spread(h), nq_ref[:, h * HD : (h + 1) * HD], preferred_element_type=jnp.float32
            )
        q_dec[...] = q_all.reshape(sessions, 8, HD)
        in_ck.wait()
        begin = (x * n_z + z) * ctx
        spot = lax.broadcasted_iota(jnp.int32, (8, ctx), 1) + begin
        scores, valid, own = [], [], []
        for s_id in range(sessions):
            q_one = q_dec[s_id]
            scores.append(
                lax.dot_general(
                    q_one.astype(jnp.bfloat16),
                    ck[s_id],
                    (((1,), (1,)), ((), ())),
                    preferred_element_type=jnp.float32,
                )
            )
            valid.append(jnp.where(spot < len_ref[s_id], 0.0, NEG))
            own.append(q_one * nk_ref[s_id : s_id + 1, :].astype(jnp.float32))
        bar = jnp.concatenate(valid, axis=0)
        s = jnp.concatenate(scores, axis=0) + bar
        own = jnp.sum(jnp.concatenate(own, axis=0), axis=1, keepdims=True)
        own = jnp.where(first_chip, own, NEG)
        m = jnp.maximum(jnp.max(s, axis=1, keepdims=True), own)
        p = jnp.where(bar < 0.0, 0.0, jnp.exp2((s - m) * scale))
        p_own = jnp.where(first_chip, jnp.exp2((own - m) * scale), 0.0)
        total = jnp.sum(p, axis=1, keepdims=True) + p_own
        p_dec[...] = p.reshape(sessions, 8, ctx)
        stat[0] = jnp.broadcast_to(m, (tall, HD))
        stat[1] = jnp.broadcast_to(total, (tall, HD))
        stat[2] = jnp.broadcast_to(p_own, (tall, HD))

    def decode_values():
        in_cv.wait()
        outs = []
        for s_id in range(sessions):
            o = jnp.dot(
                p_dec[s_id].astype(jnp.bfloat16), cv[s_id], preferred_element_type=jnp.float32
            )
            extra = stat[2, s_id * 8 : (s_id + 1) * 8, :].astype(jnp.bfloat16).astype(jnp.float32)
            outs.append(o + extra * nv_ref[s_id : s_id + 1, :].astype(jnp.float32))
        o = jnp.concatenate(outs, axis=0).reshape(sessions, 8, HD)
        m = stat[0].reshape(sessions, 8, HD)
        total = stat[1].reshape(sessions, 8, HD)
        part[...] = pack(m, total, o).reshape(part.shape)

    def exchange(number, src, dst, sem, to):
        return pltpu.make_async_remote_copy(
            src_ref=src,
            dst_ref=dst,
            send_sem=dec_send.at[number],
            recv_sem=dec_recv.at[sem],
            device_id=to,
            device_id_type=MESH,
        )

    base2, base3, base4 = n_x, n_x + quad, n_x + 2 * quad

    def round1(d):
        to = lax.rem(x + d, n_x)
        return exchange(0, part.at[to], got1.at[d - 1], d, {"seq_0": to})

    def round2(d):
        to = (z // quad) * quad + lax.rem(lax.rem(z, quad) + d, quad)
        return exchange(1, mine1, got2.at[d - 1], base2 + d, {"seq_1": to})

    def round3(d):
        to = lax.rem(z + d * quad, n_z)
        return exchange(2, mine2, got3.at[d - 1], base3 + d, {"seq_1": to})

    def round4(d):
        to = lax.rem(x + d, n_x)
        return exchange(3, last, got4.at[d - 1], base4 + d, {"seq_0": to})

    def decode_round(j):
        @pl.when(j == 1)
        def _():
            decode_scores()

        @pl.when(j == 2)
        def _():
            decode_values()

        @pl.when(j == 4)
        def _():
            for d in range(1, n_x):
                round1(d).start()

        @pl.when(j == 6)
        def _():
            for d in range(1, n_x):
                round1(d).wait_recv()
            mine1[...] = pack(*combine([part[x]] + [got1[d - 1] for d in range(1, n_x)]))

        @pl.when(j == 7)
        def _():
            for d in range(1, quad):
                round2(d).start()

        @pl.when(j == 9)
        def _():
            for d in range(1, quad):
                round2(d).wait_recv()
            mine2[...] = pack(*combine([mine1[...]] + [got2[d - 1] for d in range(1, quad)]))

        @pl.when(j == 10)
        def _():
            for d in range(1, quad):
                round3(d).start()

        @pl.when(j == 13)
        def _():
            for d in range(1, quad):
                round3(d).wait_recv()
            _, l, o = combine([mine2[...]] + [got3[d - 1] for d in range(1, quad)])
            last[...] = jnp.where(at_row[:share] == 7, 0.0, o / l)

        @pl.when(j == 14)
        def _():
            for d in range(1, n_x):
                round4(d).start()

    def receive(flow, arrivals):
        for dst, count, todo, sem in arrivals:
            pltpu.make_async_remote_copy(
                src_ref=buf.at[0, pl.ds(dst, count)],
                dst_ref=buf.at[0, pl.ds(dst, count)],
                send_sem=send_sem.at[0],
                recv_sem=recv_sem.at[sem],
                device_id=partner,
                device_id_type=MESH,
            ).wait_recv()
            for send in todo:
                ring_copy(flow, send).start()

    def receive_block(flow, j, lo, hi):
        if hi - lo == 1:
            for half in (2 * lo, 2 * lo + 1):
                receive(flow, flows[flow][2][half])
                pair_copy(half).start()
            return
        mid = (lo + hi) // 2

        @pl.when(j < mid)
        def _():
            receive_block(flow, j, lo, mid)

        @pl.when(j >= mid)
        def _():
            receive_block(flow, j, mid, hi)

    def step(j, carry):
        for flow in (0, 1):

            @pl.when(core == flow)
            def _():
                receive_block(flow, j, 0, steps)

        decode_round(j)
        attend(0, j)

        @pl.when(j > 0)
        def _():
            pair_copy(2 * j - 2).wait_recv()
            pair_copy(2 * j - 1).wait_recv()
            attend(1, j - 1)

        return carry

    lax.fori_loop(0, steps, step, 0)
    pair_copy(2 * steps - 2).wait_recv()
    pair_copy(2 * steps - 1).wait_recv()
    attend(1, steps - 1)

    for d in range(1, n_x):
        round4(d).wait_recv()
    got4[n_x - 1] = last[...]
    final = got4[...].reshape(tall, HD).astype(jnp.bfloat16)
    for h in range(GROUP):
        r = lax.broadcasted_iota(jnp.int32, (sessions, tall), 0)
        c = lax.broadcasted_iota(jnp.int32, (sessions, tall), 1)
        owner = lax.rem(x - 1 - c // (8 * share) + 2 * n_x, n_x)
        pick = (owner == r // share) & (lax.rem(c // 8, share) == lax.rem(r, share))
        pick = jnp.where(pick & (lax.rem(c, 8) == h), 1.0, 0.0).astype(jnp.bfloat16)
        row = jnp.dot(pick, final, preferred_element_type=jnp.float32)
        dec_ref[:, h * HD : (h + 1) * HD] = row.astype(jnp.bfloat16)

    def drain(number, ref):
        exchange(number, ref, ref, 0, partner).wait_send()

    drain(0, got1)
    drain(1, got2)
    drain(2, got3)
    drain(3, got4.at[pl.ds(0, n_x - 1)])
    chips = n_x * n_z
    pltpu.make_async_remote_copy(
        src_ref=buf.at[0, pl.ds(0, chips - 1)],
        dst_ref=buf.at[0, pl.ds(0, chips - 1)],
        send_sem=send_sem.at[0],
        recv_sem=recv_sem.at[0],
        device_id=partner,
        device_id_type=MESH,
    ).wait_send()
    pltpu.make_async_remote_copy(
        src_ref=buf.at[0, pl.ds(0, chips)],
        dst_ref=buf.at[1, pl.ds(0, chips)],
        send_sem=pair_send.at[0],
        recv_sem=recv_sem.at[0],
        device_id=partner,
        device_id_type=MESH,
    ).wait_send()

    me = (x * n_z + z) * 2 + core
    position = span_ref[me] * rows + lax.broadcasted_iota(jnp.int32, (rows, HD), 0)
    live = position < limit_ref[0]
    for g in range(KVH):
        for h in range(GROUP):
            head = g * GROUP + h
            at = slice(h * rows, (h + 1) * rows)
            total = jnp.sum(tot[g, at, :], axis=1, keepdims=True)
            result = jnp.where(live, acc[g, at, :] / total, 0.0)
            out_ref[:, head * HD : (head + 1) * HD] = result.astype(jnp.bfloat16)


def per_device(
    prompt_query,
    prompt_key,
    prompt_value,
    prompt_length,
    span_order,
    new_query,
    new_key,
    new_value,
    cache_key,
    cache_value,
    cache_length,
):
    rows = prompt_query.shape[0]
    n_x, n_z = lax.axis_size("seq_0"), lax.axis_size("seq_1")
    flow_a = build_flow(n_x, n_z)
    flow_b = build_flow(n_z, n_x)
    flows = (flow_a, flow_b)
    steps = len(flow_a[2]) // 2
    place_x = [a % n_x for a, _ in flow_a[0]] + [b % n_x for _, b in flow_b[0]]
    place_z = [b % n_z for _, b in flow_a[0]] + [a % n_z for a, _ in flow_b[0]]
    places = jnp.asarray(np.array(place_x + place_z, np.int32))
    width = 2 * KVH * HD
    sems = max(flow_a[3], flow_b[3])
    sessions, ctx = cache_key.shape[0], cache_key.shape[2]
    share, quad = sessions // n_x, math.isqrt(n_z)
    return pl.pallas_call(
        lambda *refs: attention_kernel(flows, (n_x, n_z), *refs),
        out_shape=(
            jax.ShapeDtypeStruct(prompt_query.shape, jnp.bfloat16),
            jax.ShapeDtypeStruct(new_query.shape, jnp.bfloat16),
        ),
        in_specs=[
            pl.BlockSpec(memory_space=pltpu.SMEM if i == 1 else pltpu.HBM) for i in range(12)
        ],
        out_specs=(
            pl.BlockSpec(memory_space=pltpu.VMEM),
            pl.BlockSpec(memory_space=pltpu.VMEM),
        ),
        scratch_shapes=[
            pltpu.VMEM((2, n_x * n_z, rows, width), jnp.bfloat16),
            pltpu.SMEM(span_order.shape, jnp.int32),
            pltpu.SMEM(places.shape, jnp.int32),
            pltpu.SMEM(cache_length.shape, jnp.int32),
            pltpu.VMEM(prompt_query.shape, jnp.bfloat16),
            pltpu.VMEM(new_query.shape, jnp.bfloat16),
            pltpu.VMEM(new_key.shape, jnp.bfloat16),
            pltpu.VMEM(new_value.shape, jnp.bfloat16),
            pltpu.VMEM((KVH, GROUP * rows, HD), jnp.bfloat16),
            pltpu.VMEM((KVH, GROUP * rows, HD), jnp.float32),
            pltpu.VMEM((KVH, GROUP * rows, HD), jnp.float32),
            pltpu.VMEM((KVH, GROUP * rows, HD), jnp.float32),
            pltpu.VMEM((sessions, ctx, HD), jnp.bfloat16),
            pltpu.VMEM((sessions, ctx, HD), jnp.bfloat16),
            pltpu.VMEM((sessions, 8, HD), jnp.float32),
            pltpu.VMEM((sessions, 8, ctx), jnp.float32),
            pltpu.VMEM((3, sessions * 8, HD), jnp.float32),
            pltpu.VMEM((n_x, share, 8, HD), jnp.float32),
            pltpu.VMEM((n_x - 1, share, 8, HD), jnp.float32),
            pltpu.VMEM((share, 8, HD), jnp.float32),
            pltpu.VMEM((quad - 1, share, 8, HD), jnp.float32),
            pltpu.VMEM((share, 8, HD), jnp.float32),
            pltpu.VMEM((quad - 1, share, 8, HD), jnp.float32),
            pltpu.VMEM((share, 8, HD), jnp.float32),
            pltpu.VMEM((n_x, share, 8, HD), jnp.float32),
            pltpu.SemaphoreType.DMA((11,)),
            pltpu.SemaphoreType.DMA((sems,)),
            pltpu.SemaphoreType.DMA((1,)),
            pltpu.SemaphoreType.DMA((2 * steps,)),
            pltpu.SemaphoreType.DMA((1,)),
            pltpu.SemaphoreType.DMA((2 * n_x + 2 * quad,)),
            pltpu.SemaphoreType.DMA((4,)),
        ],
        compiler_params=pltpu.CompilerParams(
            collective_id=0, has_side_effects=True, vmem_limit_bytes=55_000_000
        ),
        name="prefill_decode_attention",
    )(
        pltpu.with_memory_space_constraint(span_order, pltpu.HBM),
        prompt_length,
        pltpu.with_memory_space_constraint(places, pltpu.HBM),
        pltpu.with_memory_space_constraint(prompt_query, pltpu.HBM),
        pltpu.with_memory_space_constraint(prompt_key, pltpu.HBM),
        pltpu.with_memory_space_constraint(prompt_value, pltpu.HBM),
        pltpu.with_memory_space_constraint(cache_length, pltpu.HBM),
        pltpu.with_memory_space_constraint(new_query, pltpu.HBM),
        pltpu.with_memory_space_constraint(new_key, pltpu.HBM),
        pltpu.with_memory_space_constraint(new_value, pltpu.HBM),
        pltpu.with_memory_space_constraint(cache_key, pltpu.HBM),
        pltpu.with_memory_space_constraint(cache_value, pltpu.HBM),
    )


def solution(mesh):
    finer = Mesh(
        mesh.devices.reshape(mesh.shape["rep"], 8, 16, mesh.shape["head"]),
        ("rep", "seq_0", "seq_1", "head"),
    )
    placed = (
        P(REP_SEQ_HEAD, None),
        P(REP_SEQ_HEAD, None),
        P(REP_SEQ_HEAD, None),
        P("rep"),
        P("rep"),
        P("rep", "head"),
        P("rep", "head"),
        P("rep", "head"),
        P("rep", "head", SEQ, None),
        P("rep", "head", SEQ, None),
        P("rep"),
    )
    return jax.shard_map(
        per_device,
        mesh=finer,
        in_specs=placed,
        out_specs=(P(REP_SEQ_HEAD, None), P("rep", "head")),
        check_vma=False,
    )
```

```python
import functools
import heapq
import math

import jax
import jax.numpy as jnp
import numpy as np
from jax import lax
from jax.experimental import pallas as pl
from jax.experimental.pallas import tpu as pltpu
from jax.sharding import Mesh
from jax.sharding import PartitionSpec as P

HD = 128
QH = 14
KVH = 2
GROUP = QH // KVH
SEQ = ("seq_0", "seq_1")
REP_SEQ_HEAD = ("rep", "seq_0", "seq_1", "head")
TILE = 8
NEG = -1e30
MESH = pl.DeviceIdType.MESH


def build_flow(n1, n2):
    half1, half2 = n1 // 2, n2 // 2
    members = {0: [0], half1: [-half1]}
    for k in range(1, half1):
        members[k] = [-k, k]
    heap, free, seq, arrived = [], {}, [0], {}
    order, first, sends = [], [], {}

    def send(now, link, item, into):
        units = len(members[item[2]]) if item[0] == 2 else 1
        begin = max(now, free.get(link, 0.0))
        free[link] = begin + units * (0.75 if link[0] == 2 else 1.4)
        seq[0] += 1
        heapq.heappush(heap, (free[link] + 4.0, seq[0], item))
        into.append(item)

    def phase2(now, k, into):
        for way in (1, -1):
            send(now, (2, way), (2, way, k, -way), into)

    for way in (1, -1):
        send(0.0, (1, way), (1, way, -way, 0), first)
    phase2(0.0, 0, first)
    groups = [(0, 0)]
    while heap:
        now, _, item = heapq.heappop(heap)
        order.append(item)
        into = sends.setdefault(item, [])
        ring, way, which, off2 = item
        if ring == 1:
            dist, k = abs(which), abs(which)
            if dist + 1 <= (half1 if way == 1 else half1 - 1):
                send(now, (1, way), (1, way, which - way, 0), into)
            arrived[k] = arrived.get(k, 0) + 1
            if arrived[k] == len(members[k]):
                groups.append((k, 0))
                phase2(now, k, into)
        else:
            dist = abs(off2)
            groups.append((which, off2))
            last = dist + 1 == half2 and way == (1 if which % 2 == 0 else -1)
            if dist + 1 < half2 or last:
                send(now, (2, way), (2, way, which, off2 - way), into)
    slot, offsets = {}, []
    for k, off2 in groups:
        slot[(k, off2)] = len(offsets)
        offsets.extend((m, off2) for m in members[k])

    def place(item):
        ring, _, which, off2 = item
        if ring == 2:
            return slot[(which, off2)], len(members[which])
        return slot[(abs(which), 0)] + members[abs(which)].index(which), 1

    number = {item: i for i, item in enumerate(order)}

    def resolve(items):
        out = []
        for item in items:
            ring, way, which, off2 = item
            source = (1, way, which + way, 0) if ring == 1 else (2, way, which, off2 + way)
            if ring == 1 and source[2] == 0:
                src = slot[(0, 0)]
            else:
                src = place(source)[0]
            dst, count = place(item)
            out.append((ring, way, src, dst, count, number[item]))
        return out

    steps, total = [], 2 * len(offsets) // TILE
    events = [(place(item), resolve(sends[item]), number[item]) for item in order]
    at, filled = 0, {0}
    for half in range(total):
        need = set(range(half * TILE // 2, (half + 1) * TILE // 2))
        mine = []
        while not need <= filled:
            (dst, count), todo, sem = events[at]
            filled.update(range(dst, dst + count))
            mine.append((dst, count, todo, sem))
            at += 1
        steps.append(mine)
    assert at == len(events) and len(offsets) == n1 * n2
    return offsets, resolve(first), steps, len(events)


def attention_kernel(
    flows,
    sizes,
    span_hbm,
    limit_ref,
    place_hbm,
    q_hbm,
    k_ref,
    v_ref,
    len_hbm,
    nq_hbm,
    nk_hbm,
    nv_hbm,
    ck_ref,
    cv_ref,
    out_ref,
    dec_ref,
    buf,
    span_ref,
    place_ref,
    len_ref,
    q_ref,
    nq_ref,
    nk_ref,
    nv_ref,
    q_s,
    acc,
    top,
    tot,
    ck,
    cv,
    q_dec,
    p_dec,
    stat,
    part,
    got1,
    mine1,
    got2,
    mine2,
    got3,
    last,
    got4,
    local_sem,
    recv_sem,
    send_sem,
    pair_recv,
    pair_send,
    dec_recv,
    dec_send,
):
    n_x, n_z = sizes
    rows = q_ref.shape[0]
    x, z, core = lax.axis_index("seq_0"), lax.axis_index("seq_1"), lax.axis_index("head")
    steps = len(flows[0][2]) // 2
    names = ("seq_0", "seq_1")
    here = (x, z)
    extent = (n_x, n_z)

    def target(dim, way):
        return {names[dim]: lax.rem(here[dim] + way + extent[dim], extent[dim])}

    partner = {"head": 1 - core}
    barrier = pltpu.get_barrier_semaphore()
    for dim in (0, 1):
        for way in (1, -1):
            pl.semaphore_signal(barrier, inc=1, device_id=target(dim, way), device_id_type=MESH)
    pl.semaphore_signal(barrier, inc=1, device_id=partner, device_id_type=MESH)
    in_k = pltpu.make_async_copy(k_ref, buf.at[0, 0, :, : KVH * HD], local_sem.at[0])
    in_v = pltpu.make_async_copy(v_ref, buf.at[0, 0, :, KVH * HD :], local_sem.at[1])
    in_k.start()
    in_v.start()
    in_ck = pltpu.make_async_copy(ck_ref.at[:, 0], ck, local_sem.at[2])
    in_cv = pltpu.make_async_copy(cv_ref.at[:, 0], cv, local_sem.at[3])
    in_q = pltpu.make_async_copy(q_hbm, q_ref, local_sem.at[4])
    in_new = [
        pltpu.make_async_copy(src, dst, local_sem.at[5 + i])
        for i, (src, dst) in enumerate(((nq_hbm, nq_ref), (nk_hbm, nk_ref), (nv_hbm, nv_ref)))
    ]
    in_scalars = [
        pltpu.make_async_copy(src, dst, local_sem.at[8 + i])
        for i, (src, dst) in enumerate(
            ((span_hbm, span_ref), (place_hbm, place_ref), (len_hbm, len_ref))
        )
    ]
    in_q.start()
    for copy in in_scalars:
        copy.start()
    in_ck.start()
    in_cv.start()
    for copy in in_new:
        copy.start()
    in_k.wait()
    in_v.wait()
    pl.semaphore_wait(barrier, 5)

    def ring_copy(flow, send):
        ring, way, src, dst, count, sem = send
        dim = (2 - ring) if flow == 0 else (ring - 1)
        return pltpu.make_async_remote_copy(
            src_ref=buf.at[0, pl.ds(src, count)],
            dst_ref=buf.at[0, pl.ds(dst, count)],
            send_sem=send_sem.at[0],
            recv_sem=recv_sem.at[sem],
            device_id=target(dim, way),
            device_id_type=MESH,
        )

    def pair_copy(half):
        at = pl.ds(half * (TILE // 2), TILE // 2)
        return pltpu.make_async_remote_copy(
            src_ref=buf.at[0, at],
            dst_ref=buf.at[1, at],
            send_sem=pair_send.at[0],
            recv_sem=pair_recv.at[half],
            device_id=partner,
            device_id_type=MESH,
        )

    for flow in (0, 1):

        @pl.when(core == flow)
        def _():
            for send in flows[flow][1]:
                ring_copy(flow, send).start()

    scale = math.log2(math.e) / math.sqrt(HD)

    in_q.wait()
    row = lax.broadcasted_iota(jnp.int32, (rows, rows), 0)
    col = lax.broadcasted_iota(jnp.int32, (rows, rows), 1)
    tri = jnp.concatenate([jnp.where(col <= row, 0.0, NEG).astype(jnp.float32)] * GROUP, axis=0)
    for g in range(KVH):
        for h in range(GROUP):
            head = g * GROUP + h
            q_s[g, h * rows : (h + 1) * rows, :] = q_ref[:, head * HD : (head + 1) * HD]
        key = buf[0, 0, :, g * HD : (g + 1) * HD]
        value = buf[0, 0, :, (KVH + g) * HD : (KVH + g + 1) * HD]
        s = lax.dot_general(q_s[g], key, (((1,), (1,)), ((), ())), preferred_element_type=jnp.float32)
        s = s + tri
        m = jnp.max(s, axis=1, keepdims=True)
        p = jnp.exp2((s - m) * scale)
        top[g] = jnp.broadcast_to(m, (GROUP * rows, HD))
        total = jnp.sum(p, axis=1, keepdims=True)
        lane = lax.broadcasted_iota(jnp.int32, (GROUP * rows, HD), 1)
        tot[g] = jnp.where(lane == 0, total, 0.0)
        acc[g] = jnp.dot(p.astype(jnp.bfloat16), value, preferred_element_type=jnp.float32)

    keys = TILE * rows
    for copy in in_scalars:
        copy.wait()
    own_span = span_ref[(x * n_z + z) * 2 + core]

    def attend(side, tile):
        at = pl.ds(tile * TILE, TILE)
        flow = core if side == 0 else 1 - core
        marks = []
        for b in range(TILE):
            slot = flow * n_x * n_z + tile * TILE + b
            at_x = lax.rem(x + place_ref[slot], n_x)
            at_z = lax.rem(z + place_ref[2 * n_x * n_z + slot], n_z)
            span = span_ref[(at_x * n_z + at_z) * 2 + flow]
            marks.append(jnp.where(span < own_span, 0.0, NEG).astype(jnp.float32))
        lane = lax.broadcasted_iota(jnp.int32, (1, HD), 1)
        bias = []
        for b in range(0, TILE, 2):
            bias.append(jnp.where(lane < rows, marks[b], marks[b + 1]))
        bias = jnp.concatenate(bias, axis=1)
        for g in range(KVH):
            key = buf[side, at, :, g * HD : (g + 1) * HD].reshape(keys, HD)
            value = buf[side, at, :, (KVH + g) * HD : (KVH + g + 1) * HD].reshape(keys, HD)
            s = lax.dot_general(
                q_s[g], key, (((1,), (1,)), ((), ())), preferred_element_type=jnp.float32
            )
            s = s + bias
            m_old = top[g]
            m = jnp.maximum(m_old, jnp.max(s, axis=1, keepdims=True))
            factor = jnp.exp2((m_old - m) * scale)
            m_wide = jnp.concatenate([m] * (keys // HD), axis=1)
            p = jnp.exp2((s - m_wide) * scale)
            part = p[:, :HD]
            for b in range(1, keys // HD):
                part = part + p[:, b * HD : (b + 1) * HD]
            top[g] = m
            tot[g] = tot[g] * factor + part
            acc[g] = acc[g] * factor + jnp.dot(
                p.astype(jnp.bfloat16), value, preferred_element_type=jnp.float32
            )

    sessions, ctx = ck_ref.shape[0], ck_ref.shape[2]
    tall = sessions * 8
    share = sessions // n_x
    quad = math.isqrt(n_z)
    first_chip = (x == 0) & (z == 0)
    at_row = lax.broadcasted_iota(jnp.int32, (sessions, 8, HD), 1)
    at_lane = lax.broadcasted_iota(jnp.int32, (sessions, 8, HD), 2)

    def spread(h):
        r = lax.broadcasted_iota(jnp.int32, (tall, sessions), 0)
        c = lax.broadcasted_iota(jnp.int32, (tall, sessions), 1)
        return jnp.where(r == c * 8 + h, 1.0, 0.0).astype(jnp.bfloat16)

    def pack(m, l, o):
        n = o.shape[0]
        row_n, lane_n = at_row[:n], at_lane[:n]
        line = jnp.where(lane_n == row_n, m, 0.0) + jnp.where(lane_n == row_n + 8, l, 0.0)
        line = jnp.sum(line, axis=1, keepdims=True)
        return jnp.where(row_n == 7, line, o)

    def combine(tiles):
        n = tiles[0].shape[0]
        row_n, lane_n = at_row[:n], at_lane[:n]
        tops, totals = [], []
        for t in tiles:
            line = jnp.broadcast_to(t[:, 7:8, :], t.shape)
            tops.append(jnp.sum(jnp.where(lane_n == row_n, line, 0.0), axis=2, keepdims=True))
            totals.append(jnp.sum(jnp.where(lane_n == row_n + 8, line, 0.0), axis=2, keepdims=True))
        m = functools.reduce(jnp.maximum, tops)
        l, o = 0.0, 0.0
        for t, t_top, t_total in zip(tiles, tops, totals):
            f = jnp.exp2((t_top - m) * scale)
            l = l + t_total * f
            o = o + t * f
        return m, l, o

    halves = (range(sessions // 2), range(sessions // 2, sessions))

    def decode_scores(part_of):
        if part_of == 0:
            for copy in in_new:
                copy.wait()
            q_all = 0.0
            for h in range(GROUP):
                q_all = q_all + jnp.dot(
                    spread(h), nq_ref[:, h * HD : (h + 1) * HD], preferred_element_type=jnp.float32
                )
            q_dec[...] = q_all.reshape(sessions, 8, HD)
            in_ck.wait()
        for s_id in halves[part_of]:
            p_dec[s_id] = lax.dot_general(
                q_dec[s_id].astype(jnp.bfloat16),
                ck[s_id],
                (((1,), (1,)), ((), ())),
                preferred_element_type=jnp.float32,
            )

    def decode_softmax():
        begin = (x * n_z + z) * ctx
        spot = lax.broadcasted_iota(jnp.int32, (8, ctx), 1) + begin
        valid, own = [], []
        for s_id in range(sessions):
            valid.append(jnp.where(spot < len_ref[s_id], 0.0, NEG))
            own.append(q_dec[s_id] * nk_ref[s_id : s_id + 1, :].astype(jnp.float32))
        bar = jnp.concatenate(valid, axis=0)
        s = p_dec[...].reshape(tall, ctx) + bar
        own = jnp.sum(jnp.concatenate(own, axis=0), axis=1, keepdims=True)
        own = jnp.where(first_chip, own, NEG)
        m = jnp.maximum(jnp.max(s, axis=1, keepdims=True), own)
        p = jnp.where(bar < 0.0, 0.0, jnp.exp2((s - m) * scale))
        p_own = jnp.where(first_chip, jnp.exp2((own - m) * scale), 0.0)
        total = jnp.sum(p, axis=1, keepdims=True) + p_own
        p_dec[...] = p.reshape(sessions, 8, ctx)
        stat[0] = jnp.broadcast_to(m, (tall, HD))
        stat[1] = jnp.broadcast_to(total, (tall, HD))
        stat[2] = jnp.broadcast_to(p_own, (tall, HD))

    def decode_values(part_of):
        if part_of == 0:
            in_cv.wait()
        outs = []
        for s_id in halves[part_of]:
            o = jnp.dot(
                p_dec[s_id].astype(jnp.bfloat16), cv[s_id], preferred_element_type=jnp.float32
            )
            extra = stat[2, s_id * 8 : (s_id + 1) * 8, :].astype(jnp.bfloat16).astype(jnp.float32)
            outs.append(o + extra * nv_ref[s_id : s_id + 1, :].astype(jnp.float32))
        n = sessions // 2
        at = slice(part_of * n * 8, (part_of + 1) * n * 8)
        o = jnp.concatenate(outs, axis=0).reshape(n, 8, HD)
        m = stat[0, at, :].reshape(n, 8, HD)
        total = stat[1, at, :].reshape(n, 8, HD)
        to = slice(part_of * n_x // 2, (part_of + 1) * n_x // 2)
        part[to] = pack(m, total, o).reshape(n_x // 2, share, 8, HD)

    def exchange(number, src, dst, sem, to):
        return pltpu.make_async_remote_copy(
            src_ref=src,
            dst_ref=dst,
            send_sem=dec_send.at[number],
            recv_sem=dec_recv.at[sem],
            device_id=to,
            device_id_type=MESH,
        )

    base2, base3, base4 = n_x, n_x + quad, n_x + 2 * quad

    def round1(d):
        to = lax.rem(x + d, n_x)
        return exchange(0, part.at[to], got1.at[d - 1], d, {"seq_0": to})

    def round2(d):
        to = (z // quad) * quad + lax.rem(lax.rem(z, quad) + d, quad)
        return exchange(1, mine1, got2.at[d - 1], base2 + d, {"seq_1": to})

    def round3(d):
        to = lax.rem(z + d * quad, n_z)
        return exchange(2, mine2, got3.at[d - 1], base3 + d, {"seq_1": to})

    def round4(d):
        to = lax.rem(x + d, n_x)
        return exchange(3, last, got4.at[d - 1], base4 + d, {"seq_0": to})

    def send_round(one_round, count):
        for d in range(1, count):
            one_round(d).start()

    def wait_round(one_round, count):
        for d in range(1, count):
            one_round(d).wait_recv()

    def decode_round(j):
        @pl.when(j == 1)
        def _():
            decode_scores(0)

        @pl.when(j == 2)
        def _():
            decode_scores(1)

        @pl.when(j == 3)
        def _():
            decode_softmax()
            decode_values(0)

        @pl.when(j == 4)
        def _():
            decode_values(1)

        @pl.when(j == 7)
        def _():
            wait_round(round1, n_x)
            mine1[...] = pack(*combine([part[x]] + [got1[d - 1] for d in range(1, n_x)]))

        @pl.when(j == 9)
        def _():
            wait_round(round2, quad)
            mine2[...] = pack(*combine([mine1[...]] + [got2[d - 1] for d in range(1, quad)]))

        @pl.when(j == 10)
        def _():
            send_round(round3, quad)

        @pl.when(j == 13)
        def _():
            wait_round(round3, quad)
            _, l, o = combine([mine2[...]] + [got3[d - 1] for d in range(1, quad)])
            last[...] = jnp.where(at_row[:share] == 7, 0.0, o / l)

        @pl.when(j == 14)
        def _():
            send_round(round4, n_x)

    def decode_send(j):
        @pl.when(j == 4)
        def _():
            send_round(round1, n_x)

        @pl.when(j == 7)
        def _():
            send_round(round2, quad)

    def receive(flow, arrivals):
        for dst, count, todo, sem in arrivals:
            pltpu.make_async_remote_copy(
                src_ref=buf.at[0, pl.ds(dst, count)],
                dst_ref=buf.at[0, pl.ds(dst, count)],
                send_sem=send_sem.at[0],
                recv_sem=recv_sem.at[sem],
                device_id=partner,
                device_id_type=MESH,
            ).wait_recv()
            for send in todo:
                ring_copy(flow, send).start()

    def receive_block(flow, j, lo, hi):
        if hi - lo == 1:
            for half in (2 * lo, 2 * lo + 1):
                receive(flow, flows[flow][2][half])
                pair_copy(half).start()
            return
        mid = (lo + hi) // 2

        @pl.when(j < mid)
        def _():
            receive_block(flow, j, lo, mid)

        @pl.when(j >= mid)
        def _():
            receive_block(flow, j, mid, hi)

    def step(j, carry):
        for flow in (0, 1):

            @pl.when(core == flow)
            def _():
                receive_block(flow, j, 0, steps)

        decode_round(j)
        attend(0, j)

        @pl.when(j > 0)
        def _():
            pair_copy(2 * j - 2).wait_recv()
            pair_copy(2 * j - 1).wait_recv()
            attend(1, j - 1)

        decode_send(j)
        return carry

    lax.fori_loop(0, steps, step, 0)
    for d in range(1, n_x):
        round4(d).wait_recv()
    got4[n_x - 1] = last[...]
    final = got4[...].reshape(tall, HD).astype(jnp.bfloat16)
    for h in range(GROUP):
        r = lax.broadcasted_iota(jnp.int32, (sessions, tall), 0)
        c = lax.broadcasted_iota(jnp.int32, (sessions, tall), 1)
        owner = lax.rem(x - 1 - c // (8 * share) + 2 * n_x, n_x)
        pick = (owner == r // share) & (lax.rem(c // 8, share) == lax.rem(r, share))
        pick = jnp.where(pick & (lax.rem(c, 8) == h), 1.0, 0.0).astype(jnp.bfloat16)
        row = jnp.dot(pick, final, preferred_element_type=jnp.float32)
        dec_ref[:, h * HD : (h + 1) * HD] = row.astype(jnp.bfloat16)

    pair_copy(2 * steps - 2).wait_recv()
    pair_copy(2 * steps - 1).wait_recv()
    attend(1, steps - 1)

    def drain(number, ref):
        exchange(number, ref, ref, 0, partner).wait_send()

    drain(0, got1)
    drain(1, got2)
    drain(2, got3)
    drain(3, got4.at[pl.ds(0, n_x - 1)])
    chips = n_x * n_z
    pltpu.make_async_remote_copy(
        src_ref=buf.at[0, pl.ds(0, chips - 1)],
        dst_ref=buf.at[0, pl.ds(0, chips - 1)],
        send_sem=send_sem.at[0],
        recv_sem=recv_sem.at[0],
        device_id=partner,
        device_id_type=MESH,
    ).wait_send()
    pltpu.make_async_remote_copy(
        src_ref=buf.at[0, pl.ds(0, chips)],
        dst_ref=buf.at[1, pl.ds(0, chips)],
        send_sem=pair_send.at[0],
        recv_sem=recv_sem.at[0],
        device_id=partner,
        device_id_type=MESH,
    ).wait_send()

    me = (x * n_z + z) * 2 + core
    position = span_ref[me] * rows + lax.broadcasted_iota(jnp.int32, (rows, HD), 0)
    live = position < limit_ref[0]
    for g in range(KVH):
        for h in range(GROUP):
            head = g * GROUP + h
            at = slice(h * rows, (h + 1) * rows)
            total = jnp.sum(tot[g, at, :], axis=1, keepdims=True)
            result = jnp.where(live, acc[g, at, :] / total, 0.0)
            out_ref[:, head * HD : (head + 1) * HD] = result.astype(jnp.bfloat16)


def per_device(
    prompt_query,
    prompt_key,
    prompt_value,
    prompt_length,
    span_order,
    new_query,
    new_key,
    new_value,
    cache_key,
    cache_value,
    cache_length,
):
    rows = prompt_query.shape[0]
    n_x, n_z = lax.axis_size("seq_0"), lax.axis_size("seq_1")
    flow_a = build_flow(n_z, n_x)
    flow_b = build_flow(n_x, n_z)
    flows = (flow_a, flow_b)
    steps = len(flow_a[2]) // 2
    place_x = [b % n_x for _, b in flow_a[0]] + [a % n_x for a, _ in flow_b[0]]
    place_z = [a % n_z for a, _ in flow_a[0]] + [b % n_z for _, b in flow_b[0]]
    places = jnp.asarray(np.array(place_x + place_z, np.int32))
    width = 2 * KVH * HD
    sems = max(flow_a[3], flow_b[3])
    sessions, ctx = cache_key.shape[0], cache_key.shape[2]
    share, quad = sessions // n_x, math.isqrt(n_z)
    return pl.pallas_call(
        lambda *refs: attention_kernel(flows, (n_x, n_z), *refs),
        out_shape=(
            jax.ShapeDtypeStruct(prompt_query.shape, jnp.bfloat16),
            jax.ShapeDtypeStruct(new_query.shape, jnp.bfloat16),
        ),
        in_specs=[
            pl.BlockSpec(memory_space=pltpu.SMEM if i == 1 else pltpu.HBM) for i in range(12)
        ],
        out_specs=(
            pl.BlockSpec(memory_space=pltpu.VMEM),
            pl.BlockSpec(memory_space=pltpu.VMEM),
        ),
        scratch_shapes=[
            pltpu.VMEM((2, n_x * n_z, rows, width), jnp.bfloat16),
            pltpu.SMEM(span_order.shape, jnp.int32),
            pltpu.SMEM(places.shape, jnp.int32),
            pltpu.SMEM(cache_length.shape, jnp.int32),
            pltpu.VMEM(prompt_query.shape, jnp.bfloat16),
            pltpu.VMEM(new_query.shape, jnp.bfloat16),
            pltpu.VMEM(new_key.shape, jnp.bfloat16),
            pltpu.VMEM(new_value.shape, jnp.bfloat16),
            pltpu.VMEM((KVH, GROUP * rows, HD), jnp.bfloat16),
            pltpu.VMEM((KVH, GROUP * rows, HD), jnp.float32),
            pltpu.VMEM((KVH, GROUP * rows, HD), jnp.float32),
            pltpu.VMEM((KVH, GROUP * rows, HD), jnp.float32),
            pltpu.VMEM((sessions, ctx, HD), jnp.bfloat16),
            pltpu.VMEM((sessions, ctx, HD), jnp.bfloat16),
            pltpu.VMEM((sessions, 8, HD), jnp.float32),
            pltpu.VMEM((sessions, 8, ctx), jnp.float32),
            pltpu.VMEM((3, sessions * 8, HD), jnp.float32),
            pltpu.VMEM((n_x, share, 8, HD), jnp.float32),
            pltpu.VMEM((n_x - 1, share, 8, HD), jnp.float32),
            pltpu.VMEM((share, 8, HD), jnp.float32),
            pltpu.VMEM((quad - 1, share, 8, HD), jnp.float32),
            pltpu.VMEM((share, 8, HD), jnp.float32),
            pltpu.VMEM((quad - 1, share, 8, HD), jnp.float32),
            pltpu.VMEM((share, 8, HD), jnp.float32),
            pltpu.VMEM((n_x, share, 8, HD), jnp.float32),
            pltpu.SemaphoreType.DMA((11,)),
            pltpu.SemaphoreType.DMA((sems,)),
            pltpu.SemaphoreType.DMA((1,)),
            pltpu.SemaphoreType.DMA((2 * steps,)),
            pltpu.SemaphoreType.DMA((1,)),
            pltpu.SemaphoreType.DMA((2 * n_x + 2 * quad,)),
            pltpu.SemaphoreType.DMA((4,)),
        ],
        compiler_params=pltpu.CompilerParams(
            collective_id=0, has_side_effects=True, vmem_limit_bytes=55_000_000
        ),
        name="prefill_decode_attention",
    )(
        pltpu.with_memory_space_constraint(span_order, pltpu.HBM),
        prompt_length,
        pltpu.with_memory_space_constraint(places, pltpu.HBM),
        pltpu.with_memory_space_constraint(prompt_query, pltpu.HBM),
        pltpu.with_memory_space_constraint(prompt_key, pltpu.HBM),
        pltpu.with_memory_space_constraint(prompt_value, pltpu.HBM),
        pltpu.with_memory_space_constraint(cache_length, pltpu.HBM),
        pltpu.with_memory_space_constraint(new_query, pltpu.HBM),
        pltpu.with_memory_space_constraint(new_key, pltpu.HBM),
        pltpu.with_memory_space_constraint(new_value, pltpu.HBM),
        pltpu.with_memory_space_constraint(cache_key, pltpu.HBM),
        pltpu.with_memory_space_constraint(cache_value, pltpu.HBM),
    )


def solution(mesh):
    finer = Mesh(
        mesh.devices.reshape(mesh.shape["rep"], 8, 16, mesh.shape["head"]),
        ("rep", "seq_0", "seq_1", "head"),
    )
    placed = (
        P(REP_SEQ_HEAD, None),
        P(REP_SEQ_HEAD, None),
        P(REP_SEQ_HEAD, None),
        P("rep"),
        P("rep"),
        P("rep", "head"),
        P("rep", "head"),
        P("rep", "head"),
        P("rep", "head", SEQ, None),
        P("rep", "head", SEQ, None),
        P("rep"),
    )
    return jax.shard_map(
        per_device,
        mesh=finer,
        in_specs=placed,
        out_specs=(P(REP_SEQ_HEAD, None), P("rep", "head")),
        check_vma=False,
    )
```
